32 devices in a mesh: fsdp: 2 (over y), trow: 4 (over x, core), tcol: 4 (over z).
Axes of the slice: x: 2, y: 2, z: 4, core: 2. Of those that a mesh axis runs over, the one named last changes fastest.
Arguments:
- tokens: bfloat16 [512, 4096], P('fsdp', 'tcol'), may hold values from -100 to 100
- w_up: bfloat16 [4096, 16384], P('tcol', ('fsdp', 'trow')), may hold values from -0.1875 to 0.1875
- w_down: bfloat16 [16384, 4096], P(('fsdp', 'trow'), 'tcol'), may hold values from -0.046875 to 0.046875
- cotangent: bfloat16 [512, 4096], P('fsdp', 'tcol'), may hold values from -6 to 6
Outputs:
- mixed: bfloat16 [512, 4096], P('fsdp', 'tcol')
- input_gradient: bfloat16 [512, 4096], P('fsdp', 'tcol')
- grad_up: bfloat16 [4096, 16384], P('tcol', ('fsdp', 'trow'))
- grad_down: bfloat16 [16384, 4096], P(('fsdp', 'trow'), 'tcol')
The draws below stay inside these ranges and needn't reach their ends.
All inputs are finite; a program needn't handle non-finite values.
Results may differ from the reference program's by a relative error of at most 0.02.
Values may be sent and summed in bfloat16 or wider, within the bound.
A program may use at most 128 MiB of HBM per device.

```python
import jax
import jax.numpy as jnp
from jax import lax

MODEL_WIDTH = 4096
FF = 16384
TOK_GRP = 256
TOKENS = 512
N_FSDP = 2
N_TCOL = 4


def draw_tokens(key, part):
    keys = jax.random.split(jax.random.fold_in(key, 17), 3)
    rising = jnp.exp(jnp.log(3.0) * jnp.arange(MODEL_WIDTH, dtype=jnp.float32) / (MODEL_WIDTH - 1))
    column = rising * jnp.exp(jax.random.uniform(keys[1], (MODEL_WIDTH,), jnp.float32, 0.0, jnp.log(10.0))) / jnp.sqrt(30.0)
    base = jnp.clip(jax.random.normal(keys[0], (TOKENS, MODEL_WIDTH), jnp.float32), -4.0, 4.0)
    row = jnp.exp(jax.random.uniform(keys[2], (TOKENS, 1), jnp.float32, 0.0, jnp.log(10.0))) / jnp.sqrt(10.0)
    return (base * row * column[None, :]).astype(jnp.bfloat16)


def draw_w_up(key, part):
    keys = jax.random.split(jax.random.fold_in(key, 29), 2)
    position = jnp.arange(MODEL_WIDTH, dtype=jnp.float32) / (MODEL_WIDTH - 1)
    shared = jnp.clip(jax.random.normal(keys[1], (1, FF), jnp.float32), -3.0, 3.0)
    rising = jnp.exp(jnp.log(4.0) * position)
    noise = jnp.clip(jax.random.normal(keys[0], (MODEL_WIDTH, FF), jnp.float32), -4.0, 4.0)
    strength = 0.5
    rising = rising / jnp.sqrt(jnp.mean(rising * rising))
    values = rising[:, None] * (noise + strength * shared) / jnp.sqrt(1.0 * MODEL_WIDTH)
    return values.astype(jnp.bfloat16)


def shard_levels(own_key, dims, cuts, low, high):
    def one(dim, parts):
        steps = jax.random.uniform(jax.random.fold_in(jax.random.fold_in(own_key, 6), dim), (parts,), jnp.float32, low / len(cuts), high / len(cuts))
        return jnp.repeat(jnp.exp(steps), dims[dim] // parts).reshape((-1,) + (1,) * (len(dims) - dim - 1))

    level = one(*cuts[0])
    for cut in cuts[1:]:
        level = level * one(*cut)
    return level


def bell_draw(stream_key, shape, spread, reach, shards=(), kind=jnp.bfloat16):
    result = spread * jax.random.normal(stream_key, shape, jnp.float32)
    if shards:
        result = result * shard_levels(stream_key, shape, shards, -0.22, 0.18)
    return jnp.clip(result, -reach, reach).astype(kind)


def setup_inputs(seed: int = 0) -> dict:
    key_of = jax.random.split(jax.random.key(seed), 5)
    return {
        "tokens": draw_tokens(jax.random.fold_in(key_of[4], 71), 0),
        "w_up": draw_w_up(jax.random.fold_in(key_of[4], 71), 0),
        "w_down": bell_draw(key_of[2], (FF, MODEL_WIDTH), FF ** -0.5, 0.046875, ((0, 8), (1, 4))),
        "cotangent": bell_draw(key_of[3], (TOKENS, MODEL_WIDTH), 1.0, 6.0, ((0, 2), (1, 4))),
    }


def gelu_value(pre):
    phi = 0.5 * (1.0 + jax.scipy.special.erf(pre * 0.7071067811865476))
    return pre * phi

def gelu_slope(pre):
    phi = 0.5 * (1.0 + jax.scipy.special.erf(pre * 0.7071067811865476))
    return phi + pre * jnp.exp(-0.5 * pre * pre) * 0.3989422804014327

def rounded_term(value):
    low = lax.optimization_barrier(value.astype(jnp.bfloat16))
    return low.astype(jnp.float32)

def reference(tokens, w_up, w_down, cotangent):
    block = MODEL_WIDTH // N_TCOL
    input_float = tokens.astype(jnp.float32)
    token_mean = lax.optimization_barrier(jnp.sum(input_float, axis=1)) / MODEL_WIDTH
    var = lax.optimization_barrier(jnp.sum(input_float * input_float, axis=1)) / MODEL_WIDTH - token_mean * token_mean
    inverse_stddev = lax.rsqrt(var + 1e-05)
    centered_scaled = (input_float - token_mean[:, None]) * inverse_stddev[:, None]
    normalized_rows = centered_scaled.astype(jnp.bfloat16)

    def pre_step(index, total):
        start = (index * block).astype(jnp.int32)
        left = lax.dynamic_slice_in_dim(normalized_rows, start, block, 1)
        right = lax.dynamic_slice_in_dim(w_up, start, block, 0)
        return total + rounded_term(jnp.dot(left, right, preferred_element_type=jnp.float32))
    pre = lax.fori_loop(0, N_TCOL, pre_step, jnp.zeros((TOKENS, FF), jnp.float32))
    hidden = gelu_value(pre).astype(jnp.bfloat16)
    branch = jnp.dot(hidden, w_down, preferred_element_type=jnp.float32)
    mixed = (input_float + branch).astype(jnp.bfloat16)

    def down_step(index, total):
        start = (index * TOK_GRP).astype(jnp.int32)
        left = lax.dynamic_slice_in_dim(hidden, start, TOK_GRP, 0)
        right = lax.dynamic_slice_in_dim(cotangent, start, TOK_GRP, 0)
        part = lax.dot_general(left, right, (((0,), (0,)), ((), ())), preferred_element_type=jnp.float32)
        return total + rounded_term(part)
    grad_down = lax.fori_loop(0, N_FSDP, down_step, jnp.zeros((FF, MODEL_WIDTH), jnp.float32))

    def dh_step(index, total):
        start = (index * block).astype(jnp.int32)
        left = lax.dynamic_slice_in_dim(cotangent, start, block, 1)
        right = lax.dynamic_slice_in_dim(w_down, start, block, 1)
        part = lax.dot_general(left, right, (((1,), (1,)), ((), ())), preferred_element_type=jnp.float32)
        return total + rounded_term(part)
    dhid = lax.fori_loop(0, N_TCOL, dh_step, jnp.zeros((TOKENS, FF), jnp.float32))
    dpre = (dhid * gelu_slope(pre)).astype(jnp.bfloat16)

    def up_step(index, total):
        start = (index * TOK_GRP).astype(jnp.int32)
        left = lax.dynamic_slice_in_dim(normalized_rows, start, TOK_GRP, 0)
        right = lax.dynamic_slice_in_dim(dpre, start, TOK_GRP, 0)
        part = lax.dot_general(left, right, (((0,), (0,)), ((), ())), preferred_element_type=jnp.float32)
        return total + rounded_term(part)
    grad_up = lax.fori_loop(0, N_FSDP, up_step, jnp.zeros((MODEL_WIDTH, FF), jnp.float32))
    normed_gradient = lax.dot_general(dpre, w_up, (((1,), (1,)), ((), ())), preferred_element_type=jnp.float32)
    first_moment = lax.optimization_barrier(jnp.sum(normed_gradient, axis=1)) / MODEL_WIDTH
    second_moment = lax.optimization_barrier(jnp.sum(normed_gradient * centered_scaled, axis=1)) / MODEL_WIDTH
    input_gradient = cotangent.astype(jnp.float32) + inverse_stddev[:, None] * (normed_gradient - first_moment[:, None] - centered_scaled * second_moment[:, None])
    return (mixed, input_gradient.astype(jnp.bfloat16), grad_up.astype(jnp.bfloat16), grad_down.astype(jnp.bfloat16))
```

```python
import functools

import jax
import jax.numpy as jnp
from jax import lax
from jax.experimental import pallas as pl
from jax.experimental.pallas import tpu as pltpu
from jax.sharding import PartitionSpec as P

MESH = pl.DeviceIdType.MESH
BF16 = jnp.bfloat16
F32 = jnp.float32
SQRT_HALF = 0.7071067811865476
INV_SQRT_2PI = 0.3989422804014327
EPS = 1e-05
END_LAG = 9
MID_LAG = 2


def gelu_value(pre):
    phi = 0.5 * (1.0 + jax.scipy.special.erf(pre * SQRT_HALF))
    return pre * phi


def gelu_slope(pre):
    phi = 0.5 * (1.0 + jax.scipy.special.erf(pre * SQRT_HALF))
    return phi + pre * jnp.exp(-0.5 * pre * pre) * INV_SQRT_2PI


def contract(left, right, left_dim, right_dim):
    return lax.dot_general(
        left, right, (((left_dim,), (right_dim,)), ((), ())), preferred_element_type=F32
    )


def line_kernel(
    sizes,
    tok_in, up_in, down_in, cot_in,
    mixed_out, grad_out, hid_out, dpre_out, norm_out, cot_out,
    xall, call, nall, wu, wd, tx, rx, rm, hd,
    st_tx, st_rx, flip, ms, acc, rs_tx, rs_rx, keep, y_tx, y_rx, ag_rx, mix_v, st2, f_tx, f_rx, ig_v,
    load_sem, wu_sem, wd_sem, tx_sem, rx_sem, rm_sem, hs_sem, hr_sem, ho_sem,
    ss_sem, sr_sem, ys_sem, yr_sem, rss_sem, rsr_sem, yqs_sem, yqr_sem, ags_sem, agr_sem,
    fs_sem, fr_sem, out_sem,
):
    nz, nt, rows, depth, ff, tb_size, fb_size = sizes
    nfb = ff // fb_size
    ntb = 2 * rows // tb_size
    half = ntb // 2
    nb = ntb * nfb
    quarter = depth // nt
    width = depth * nz
    y = lax.axis_index("fsdp")
    tr = lax.axis_index("trow")
    j = lax.axis_index("tcol")
    mid_low = nz // 2 - 1
    is_mid = jnp.logical_or(j == mid_low, j == mid_low + 1)
    is_end = jnp.logical_not(is_mid)
    inner = jnp.where(j <= mid_low, j + 1, j - 1)
    outer = jnp.where(j <= mid_low, jnp.maximum(j - 1, 0), jnp.minimum(j + 1, nz - 1))
    lag = jnp.where(is_mid, MID_LAG, END_LAG)

    def at(yy, tt, jj):
        return {"fsdp": yy, "trow": tt, "tcol": jj}

    def remote(src, dst, send, recv, device):
        return pltpu.make_async_remote_copy(
            src_ref=src, dst_ref=dst, send_sem=send, recv_sem=recv,
            device_id=device, device_id_type=MESH,
        )

    def z_peer(d):
        return lax.rem(j + d, nz)

    def t_peer(d):
        return lax.rem(tr + d, nt)

    here = at(y, tr, j)
    other = 1 - y

    own = pl.ds(0, rows)
    far = pl.ds(rows, rows)
    tok_load = pltpu.make_async_copy(tok_in, xall.at[own], load_sem.at[0])
    cot_load = pltpu.make_async_copy(cot_in, call.at[own], load_sem.at[1])

    def wd_load(f):
        return pltpu.make_async_copy(
            down_in.at[pl.ds(pl.multiple_of(f * fb_size, fb_size), fb_size)], wd.at[f], wd_sem.at[f]
        )

    def wu_load(f):
        return pltpu.make_async_copy(
            up_in.at[:, pl.ds(pl.multiple_of(f * fb_size, fb_size), fb_size)], wu.at[f], wu_sem.at[f]
        )

    tok_load.start()
    cot_load.start()
    for f in range(nfb):
        wd_load(f).start()
        wu_load(f).start()

    barrier = pltpu.get_barrier_semaphore()
    partners = [at(y, tr, z_peer(d)) for d in range(1, nz)]
    partners += [at(other, tr, z_peer(d)) for d in range(nz)]
    partners += [at(y, t_peer(d), j) for d in range(1, nt)]
    for device in partners:
        pl.semaphore_signal(barrier, inc=1, device_id=device, device_id_type=MESH)
    pl.semaphore_wait(barrier, len(partners))

    lane = lax.broadcasted_iota(jnp.int32, (tb_size, 128), 1)

    def pair_tile(one, two):
        return jnp.where(lane == 0, one, jnp.where(lane == 1, two, 0.0))

    tok_load.wait()

    def stat_step(i, carry):
        at_rows = pl.ds(pl.multiple_of(i * tb_size, tb_size), tb_size)
        x = xall[at_rows, :].astype(F32)
        st2[at_rows, :] = pair_tile(
            jnp.sum(x, axis=1, keepdims=True), jnp.sum(x * x, axis=1, keepdims=True)
        )
        return carry

    lax.fori_loop(0, half, stat_step, 0)
    stats = st2[...].T[0:8]
    st_tx[...] = stats
    st_rx[0, j] = stats

    def stat_copy(k, rel, d):
        target = at(y if rel == 0 else other, tr, z_peer(d))
        return remote(st_tx, st_rx.at[rel, j], ss_sem.at[k], sr_sem.at[rel, d], target)

    stat_list = [(0, d) for d in range(1, nz)] + [(1, d) for d in range(nz)]
    for k, (rel, d) in enumerate(stat_list):
        stat_copy(k, rel, d).start()
    cot_load.wait()
    y_cot = remote(call.at[own], call.at[far], ys_sem.at[0], yr_sem.at[0], at(other, tr, j))
    y_tok = remote(xall.at[own], xall.at[far], ys_sem.at[1], yr_sem.at[1], at(other, tr, j))
    y_cot.start()
    y_tok.start()

    def normalize(rel):
        for d in range(1 if rel == 0 else 0, nz):
            source = lax.rem(j + nz - d, nz)
            remote(st_tx, st_rx.at[rel, source], ss_sem.at[0], sr_sem.at[rel, d], here).wait_recv()
        total = st_rx[rel, 0]
        for z in range(1, nz):
            total = total + st_rx[rel, z]
        total = total / width
        mean = total[0:1]
        rstd = lax.rsqrt(total[1:2] - mean * mean + EPS)
        flip[...] = jnp.zeros_like(flip)
        flip[0:1] = mean
        flip[1:2] = rstd
        back = flip[...].T
        ms[rel] = back

        def step(i, carry):
            in_rows = pl.ds(pl.multiple_of(i * tb_size, tb_size), tb_size)
            at_rows = pl.ds(pl.multiple_of(rel * rows + i * tb_size, tb_size), tb_size)
            x = xall[at_rows, :].astype(F32)
            tile = ms[rel, in_rows, :]
            nall[at_rows, :] = ((x - tile[:, 0:1]) * tile[:, 1:2]).astype(BF16)
            return carry

        lax.fori_loop(0, half, step, 0)
        span = own if rel == 0 else far
        pltpu.make_async_copy(nall.at[span], norm_out.at[span], out_sem.at[rel]).start()
        pltpu.make_async_copy(call.at[span], cot_out.at[span], out_sem.at[2 + rel]).start()

    def inward(k, s):
        return (
            remote(tx.at[k, s], rx.at[k, s], tx_sem.at[k, s], rx_sem.at[k, s], at(y, tr, inner)),
            remote(tx.at[k, s], rm.at[k, s], tx_sem.at[k, s], rm_sem.at[k, s], at(y, tr, inner)),
        )

    def outward(k, s):
        return remote(hd.at[k, s], hd.at[k, s], hs_sem.at[k, s], hr_sem.at[k, s], at(y, tr, outer))

    def send_partial(k, s, part):
        to_mid, across = inward(k, s)

        @pl.when(is_end)
        def _():
            tx[k, s] = part.astype(BF16)
            to_mid.start()

        @pl.when(is_mid)
        def _():
            to_mid.wait_recv()
            tx[k, s] = (part + rx[k, s].astype(F32)).astype(BF16)
            across.start()

    def block_rows(t):
        return pl.ds(pl.multiple_of(t * tb_size, tb_size), tb_size)

    def partial_stage(s):
        t = s // nfb
        f = lax.rem(s, nfb)

        @pl.when(s < nfb)
        def _():
            wd_load(f).wait()
            wu_load(f).wait()

        @pl.when(s == nb // 2)
        def _():
            y_cot.wait_recv()
            y_tok.wait_recv()
            normalize(1)

        send_partial(0, s, contract(call[block_rows(t), :], wd[f], 1, 1))

        @pl.when(s == 0)
        def _():
            normalize(0)

        send_partial(1, s, contract(nall[block_rows(t), :], wu[f], 1, 0))

    def act_stage(e):
        for k in range(2):
            inward(k, e)[1].wait_recv()

        def step(i, carry):
            r = pl.ds(pl.multiple_of(i * 16, 16), 16)
            dhid = tx[0, e, r, :].astype(F32) + rm[0, e, r, :].astype(F32)
            pre = tx[1, e, r, :].astype(F32) + rm[1, e, r, :].astype(F32)
            phi = 0.5 * (1.0 + lax.erf(pre * SQRT_HALF))
            slope = phi + pre * jnp.exp(-0.5 * pre * pre) * INV_SQRT_2PI
            hd[0, e, r, :] = (pre * phi).astype(BF16)
            hd[1, e, r, :] = (dhid * slope).astype(BF16)
            return carry

        lax.fori_loop(0, tb_size // 16, step, 0)
        for k in range(2):
            outward(k, e).start()

    def hbm_copy(k, e):
        out = hid_out if k == 0 else dpre_out
        cols = pl.ds(pl.multiple_of(lax.rem(e, nfb) * fb_size, fb_size), fb_size)
        return pltpu.make_async_copy(hd.at[k, e], out.at[block_rows(e // nfb), cols], ho_sem.at[k, e])

    def rs_copy(t, d):
        return remote(
            rs_tx.at[t, d - 1], rs_rx.at[t, d - 1], rss_sem.at[t, d - 1], rsr_sem.at[t, d - 1],
            at(y, t_peer(d), j),
        )

    def columns(q):
        return pl.ds(pl.multiple_of(q * quarter, quarter), quarter)

    def use_stage(e):
        @pl.when(is_end)
        def _():
            for k in range(2):
                outward(k, e).wait_recv()

        for k in range(2):
            hbm_copy(k, e).start()
        f = lax.rem(e, nfb)
        t = e // nfb

        @pl.when(f == 0)
        def _():
            acc[...] = jnp.zeros_like(acc)

        acc[0] += contract(hd[0, e], wd[f], 1, 0)
        acc[1] += contract(hd[1, e], wu[f], 1, 1)

        @pl.when(f == nfb - 1)
        def _():
            for d in range(1, nt):
                for k in range(2):
                    rs_tx[t, d - 1, k] = acc[k, :, columns(t_peer(d))].astype(BF16)
                rs_copy(t, d).start()
            for k in range(2):
                keep[t, k] = acc[k, :, columns(tr)]

    def yq_copy(t):
        return remote(y_tx.at[t], y_rx.at[t], yqs_sem.at[t], yqr_sem.at[t], at(other, tr, j))

    def ag_copy(t, d):
        return remote(
            ag_rx.at[t, tr], ag_rx.at[t, tr], ags_sem.at[t, d - 1], agr_sem.at[t, d - 1],
            at(y, t_peer(d), j),
        )

    def row_sum_stage(t):
        for d in range(1, nt):
            rs_copy(t, d).wait_recv()
        for k in range(2):
            total = keep[t, k]
            for d in range(1, nt):
                total = total + rs_rx[t, d - 1, k].astype(F32)
            keep[t, k] = total

        @pl.when(t >= half)
        def _():
            for k in range(2):
                y_tx[t - half, k] = keep[t, k].astype(BF16)
            yq_copy(t - half).start()

    def gather_stage(t):
        yq_copy(t).wait_recv()
        for k in range(2):
            ag_rx[t, tr, k] = (keep[t, k] + y_rx[t, k].astype(F32)).astype(BF16)
        for d in range(1, nt):
            ag_copy(t, d).start()

    def xhat_of(t, q):
        tile = ms[0, block_rows(t), :]
        x = xall[block_rows(t), q * quarter:(q + 1) * quarter].astype(F32)
        return x, (x - tile[:, 0:1]) * tile[:, 1:2]

    def finish_stage(t):
        for d in range(1, nt):
            source = lax.rem(tr + nt - d, nt)
            remote(
                ag_rx.at[t, source], ag_rx.at[t, source], ags_sem.at[t, d - 1],
                agr_sem.at[t, d - 1], here,
            ).wait_recv()
        one = jnp.zeros((tb_size, 1), F32)
        two = jnp.zeros((tb_size, 1), F32)
        for q in range(nt):
            x, xhat = xhat_of(t, q)
            mix_v[block_rows(t), q * quarter:(q + 1) * quarter] = (
                x + ag_rx[t, q, 0].astype(F32)
            ).astype(BF16)
            dn = ag_rx[t, q, 1].astype(F32)
            one += jnp.sum(dn, axis=1, keepdims=True)
            two += jnp.sum(dn * xhat, axis=1, keepdims=True)
        st2[block_rows(t), :] = pair_tile(one, two)

    def step(s, carry):
        @pl.when(s < nb)
        def _():
            partial_stage(s)

        e = s - lag
        valid = jnp.logical_and(e >= 0, e < nb)

        @pl.when(jnp.logical_and(valid, is_mid))
        def _():
            act_stage(e)

        @pl.when(valid)
        def _():
            use_stage(e)

        def done_block(shift, low, high, stage):
            k = e - shift - (nfb - 1)
            t = k // nfb
            ok = jnp.logical_and(k >= low * nfb, k < high * nfb)

            @pl.when(jnp.logical_and(ok, lax.rem(k, nfb) == 0))
            def _():
                stage(t - low if low else t)

        done_block(2, 0, ntb, row_sum_stage)
        done_block(4, half, ntb, gather_stage)
        done_block(6, half, ntb, finish_stage)
        return carry

    lax.fori_loop(0, nb + max(END_LAG, MID_LAG) + 6, step, 0)

    pltpu.make_async_copy(mix_v, mixed_out, out_sem.at[4]).start()

    stats = st2[...].T[0:8]
    f_tx[...] = stats
    f_rx[j] = stats

    def f_copy(d):
        return remote(f_tx, f_rx.at[j], fs_sem.at[d - 1], fr_sem.at[d - 1], at(y, tr, z_peer(d)))

    for d in range(1, nz):
        f_copy(d).start()
    for d in range(1, nz):
        source = lax.rem(j + nz - d, nz)
        remote(f_tx, f_rx.at[source], fs_sem.at[d - 1], fr_sem.at[d - 1], here).wait_recv()
    total = f_rx[0]
    for z in range(1, nz):
        total = total + f_rx[z]
    flip[0:8] = total / width
    st2[...] = flip[...].T

    def last_step(t, carry):
        tile = st2[block_rows(t), :]
        rstd = ms[0, block_rows(t), :][:, 1:2]
        for q in range(nt):
            span = slice(q * quarter, (q + 1) * quarter)
            _, xhat = xhat_of(t, q)
            dn = ag_rx[t, q, 1].astype(F32)
            ig_v[block_rows(t), span] = (
                call[block_rows(t), span].astype(F32)
                + rstd * (dn - tile[:, 0:1] - xhat * tile[:, 1:2])
            ).astype(BF16)
        return carry

    lax.fori_loop(0, half, last_step, 0)
    pltpu.make_async_copy(ig_v, grad_out, out_sem.at[5]).start()

    for k, (rel, d) in enumerate(stat_list):
        stat_copy(k, rel, d).wait_send()
    y_cot.wait_send()
    y_tok.wait_send()

    def drain_block(s, carry):
        for k in range(2):
            inward(k, s)[0].wait_send()
            hbm_copy(k, s).wait()
        return carry

    lax.fori_loop(0, nb, drain_block, 0)

    @pl.when(is_mid)
    def _():
        def drain_out(s, carry):
            for k in range(2):
                outward(k, s).wait_send()
            return carry

        lax.fori_loop(0, nb, drain_out, 0)

    def drain_rows(t, carry):
        for d in range(1, nt):
            rs_copy(t, d).wait_send()
        return carry

    lax.fori_loop(0, ntb, drain_rows, 0)

    def drain_half(t, carry):
        yq_copy(t).wait_send()
        for d in range(1, nt):
            ag_copy(t, d).wait_send()
        return carry

    lax.fori_loop(0, half, drain_half, 0)
    for d in range(1, nz):
        f_copy(d).wait_send()
    pltpu.make_async_copy(mix_v, mixed_out, out_sem.at[4]).wait()
    pltpu.make_async_copy(ig_v, grad_out, out_sem.at[5]).wait()
    for rel, span in enumerate((own, far)):
        pltpu.make_async_copy(nall.at[span], norm_out.at[span], out_sem.at[rel]).wait()
        pltpu.make_async_copy(call.at[span], cot_out.at[span], out_sem.at[2 + rel]).wait()


def line_call(nz, nt, tokens, w_up, w_down, cotangent):
    rows, depth = tokens.shape
    ff = w_up.shape[1]
    tb, fb = 64, 512
    nfb = ff // fb
    ntb = 2 * rows // tb
    half = ntb // 2
    nb = nfb * ntb
    quarter = depth // nt
    vm = pltpu.VMEM
    dma = pltpu.SemaphoreType.DMA
    big = (2, nb, tb, fb)
    scratch = [
        vm((2 * rows, depth), BF16), vm((2 * rows, depth), BF16), vm((2 * rows, depth), BF16),
        vm((nfb, depth, fb), BF16), vm((nfb, fb, depth), BF16),
        vm(big, BF16), vm(big, BF16), vm(big, BF16), vm(big, BF16),
        vm((8, rows), F32), vm((2, nz, 8, rows), F32), vm((128, rows), F32), vm((2, rows, 128), F32),
        vm((2, tb, depth), F32),
        vm((ntb, nt - 1, 2, tb, quarter), BF16), vm((ntb, nt - 1, 2, tb, quarter), BF16),
        vm((ntb, 2, tb, quarter), F32),
        vm((half, 2, tb, quarter), BF16), vm((half, 2, tb, quarter), BF16),
        vm((half, nt, 2, tb, quarter), BF16),
        vm((rows, depth), BF16), vm((rows, 128), F32),
        vm((8, rows), F32), vm((nz, 8, rows), F32), vm((rows, depth), BF16),
        dma((2,)), dma((nfb,)), dma((nfb,)),
        dma((2, nb)), dma((2, nb)), dma((2, nb)), dma((2, nb)), dma((2, nb)), dma((2, nb)),
        dma((2 * nz - 1,)), dma((2, nz)), dma((2,)), dma((2,)),
        dma((ntb, nt - 1)), dma((ntb, nt - 1)), dma((half,)), dma((half,)),
        dma((half, nt - 1)), dma((half, nt - 1)),
        dma((nz - 1,)), dma((nz - 1,)), dma((6,)),
    ]
    any_spec = pl.BlockSpec(memory_space=pl.ANY)
    out = lambda *shape: jax.ShapeDtypeStruct(shape, BF16)
    return pl.pallas_call(
        functools.partial(line_kernel, (nz, nt, rows, depth, ff, tb, fb)),
        out_shape=(
            out(rows, depth), out(rows, depth), out(2 * rows, ff), out(2 * rows, ff),
            out(2 * rows, depth), out(2 * rows, depth),
        ),
        in_specs=[any_spec] * 4,
        out_specs=[any_spec] * 6,
        scratch_shapes=scratch,
        compiler_params=pltpu.CompilerParams(
            collective_id=0, has_side_effects=True, vmem_limit_bytes=56 * 1024 * 1024
        ),
    )(tokens, w_up, w_down, cotangent)


def local_line(tokens, w_up, w_down, cotangent):
    nz = lax.axis_size("tcol")
    nt = lax.axis_size("trow")
    mixed, grad, hidden, dpre, normed, cot = line_call(nz, nt, tokens, w_up, w_down, cotangent)
    grad_down = contract(hidden, cot, 0, 0).astype(BF16)
    grad_up = contract(normed, dpre, 0, 0).astype(BF16)
    return mixed, grad, grad_up, grad_down


def local_plain(tokens, w_up, w_down, cotangent):
    width = tokens.shape[1] * lax.axis_size("tcol")
    input_float = tokens.astype(F32)
    cot_all = lax.all_gather(cotangent, "fsdp", axis=0, tiled=True)
    sum_one, sum_two = lax.psum(
        (jnp.sum(input_float, axis=1), jnp.sum(input_float * input_float, axis=1)), "tcol"
    )
    token_mean = sum_one / width
    var = sum_two / width - token_mean * token_mean
    inverse_stddev = lax.rsqrt(var + EPS)
    centered_scaled = (input_float - token_mean[:, None]) * inverse_stddev[:, None]
    normalized_rows = centered_scaled.astype(BF16)
    normed_all = lax.all_gather(normalized_rows, "fsdp", axis=0, tiled=True)
    dhid_part = contract(cot_all, w_down, 1, 1).astype(BF16)
    dhid = lax.psum_scatter(dhid_part, "tcol", scatter_dimension=0, tiled=True).astype(F32)
    pre_part = contract(normed_all, w_up, 1, 0).astype(BF16)
    pre = lax.psum_scatter(pre_part, "tcol", scatter_dimension=0, tiled=True).astype(F32)
    hidden = lax.all_gather(gelu_value(pre).astype(BF16), "tcol", axis=0, tiled=True)
    dpre = lax.all_gather((dhid * gelu_slope(pre)).astype(BF16), "tcol", axis=0, tiled=True)
    branch_part = contract(hidden, w_down, 1, 0).astype(BF16)
    branch = lax.psum_scatter(branch_part, "fsdp", scatter_dimension=0, tiled=True)
    branch = lax.psum(branch, "trow").astype(F32)
    mixed = (input_float + branch).astype(BF16)
    grad_down = contract(hidden, cot_all, 0, 0).astype(BF16)
    dnorm_part = contract(dpre, w_up, 1, 1).astype(BF16)
    dnorm = lax.psum_scatter(dnorm_part, "fsdp", scatter_dimension=0, tiled=True)
    normed_gradient = lax.psum(dnorm, "trow").astype(F32)
    grad_up = contract(normed_all, dpre, 0, 0).astype(BF16)
    mean_first, mean_second = lax.psum(
        (jnp.sum(normed_gradient, axis=1), jnp.sum(normed_gradient * centered_scaled, axis=1)),
        "tcol",
    )
    first_moment = mean_first / width
    second_moment = mean_second / width
    input_gradient = cotangent.astype(F32) + inverse_stddev[:, None] * (
        normed_gradient - first_moment[:, None] - centered_scaled * second_moment[:, None]
    )
    return (mixed, input_gradient.astype(BF16), grad_up, grad_down)


def solution(mesh):
    fits = mesh.shape["fsdp"] == 2 and mesh.shape["tcol"] == 4
    return jax.shard_map(
        local_line if fits else local_plain,
        mesh=mesh,
        in_specs=(
            P("fsdp", "tcol"),
            P("tcol", ("fsdp", "trow")),
            P(("fsdp", "trow"), "tcol"),
            P("fsdp", "tcol"),
        ),
        out_specs=(
            P("fsdp", "tcol"),
            P("fsdp", "tcol"),
            P("tcol", ("fsdp", "trow")),
            P(("fsdp", "trow"), "tcol"),
        ),
        check_vma=False,
    )
```

```python
import functools

import jax
import jax.numpy as jnp
from jax import lax
from jax.experimental import pallas as pl
from jax.experimental.pallas import tpu as pltpu
from jax.sharding import PartitionSpec as P

MESH = pl.DeviceIdType.MESH
BF16 = jnp.bfloat16
F32 = jnp.float32
SQRT_HALF = 0.7071067811865476
INV_SQRT_2PI = 0.3989422804014327
EPS = 1e-05
END_LAG = 16
MID_LAG = 3
ROW_SHIFT = 5
FB_SIZE = 256
VMEM_LIMIT = 46 * 1024 * 1024
WRITE_LIMIT = 1024 * 1024
OUT = pltpu.VMEM


def gelu_value(pre):
    phi = 0.5 * (1.0 + jax.scipy.special.erf(pre * SQRT_HALF))
    return pre * phi


def gelu_slope(pre):
    phi = 0.5 * (1.0 + jax.scipy.special.erf(pre * SQRT_HALF))
    return phi + pre * jnp.exp(-0.5 * pre * pre) * INV_SQRT_2PI


def contract(left, right, left_dim, right_dim):
    return lax.dot_general(
        left, right, (((left_dim,), (right_dim,)), ((), ())), preferred_element_type=F32
    )


def line_kernel(
    sizes,
    tok_in, up_in, down_in, cot_in,
    mixed, grad, grad_up, grad_down,
    xall, call, nall, wu, wd, tx, rx, rm, hd,
    st_own, st_tx, st_rx, flip, ms, acc, rs_tx, rs_rx, keep, y_tx, y_rx, ag_rx, square, sq_tx, sq_rx,
    load_sem, wu_sem, wd_sem, tx_sem, rx_sem, rm_sem, hs_sem, hr_sem,
    ss_sem, sr_sem, ys_sem, yr_sem, rss_sem, rsr_sem, yqs_sem, yqr_sem, ags_sem, agr_sem,
    sqs_sem, sqr_sem,
):
    nz, nt, rows, depth, ff, tb_size, fb_size = sizes
    nfb = ff // fb_size
    ntb = 2 * rows // tb_size
    half = ntb // 2
    lead = half // 2
    nb = ntb * nfb
    quarter = depth // nt
    width = depth * nz
    y = lax.axis_index("fsdp")
    tr = lax.axis_index("trow")
    j = lax.axis_index("tcol")
    mid_low = nz // 2 - 1
    is_mid = jnp.logical_or(j == mid_low, j == mid_low + 1)
    is_end = jnp.logical_not(is_mid)
    inner = jnp.where(j <= mid_low, j + 1, j - 1)
    outer = jnp.where(j <= mid_low, jnp.maximum(j - 1, 0), jnp.minimum(j + 1, nz - 1))
    lag = jnp.where(is_mid, MID_LAG, END_LAG)
    other = 1 - y

    def at(yy, tt, jj):
        return {"fsdp": yy, "trow": tt, "tcol": jj}

    def remote(src, dst, send, recv, device):
        return pltpu.make_async_remote_copy(
            src_ref=src, dst_ref=dst, send_sem=send, recv_sem=recv,
            device_id=device, device_id_type=MESH,
        )

    def z_peer(d):
        return lax.rem(j + d, nz)

    def t_peer(d):
        return lax.rem(tr + d, nt)

    here = at(y, tr, j)

    def own_block(o):
        return o if o < lead else o + half

    def block_rows(t):
        return pl.ds(pl.multiple_of(t * tb_size, tb_size), tb_size)

    head = lead * tb_size
    spans = [(pl.ds(0, head), pl.ds(0, head)), (pl.ds(head, rows - head), pl.ds(head + rows, rows - head))]

    def own_load(which, part):
        source, dest = (tok_in, xall) if which == 0 else (cot_in, call)
        return pltpu.make_async_copy(
            source.at[spans[part][0]], dest.at[spans[part][1]], load_sem.at[which, part]
        )

    def wd_load(f):
        return pltpu.make_async_copy(
            down_in.at[pl.ds(pl.multiple_of(f * fb_size, fb_size), fb_size)], wd.at[f], wd_sem.at[f]
        )

    def wu_load(f):
        return pltpu.make_async_copy(
            up_in.at[:, pl.ds(pl.multiple_of(f * fb_size, fb_size), fb_size)], wu.at[f], wu_sem.at[f]
        )

    for part in range(2):
        own_load(0, part).start()
    for part in range(2):
        own_load(1, part).start()
    for f in range(nfb):
        wd_load(f).start()
        wu_load(f).start()

    barrier = pltpu.get_barrier_semaphore()
    partners = [(y, t_peer(a), z_peer(b)) for a in range(nt) for b in range(nz) if a or b]
    partners += [(other, tr, z_peer(b)) for b in range(nz)]
    for device in partners:
        pl.semaphore_signal(barrier, inc=1, device_id=at(*device), device_id_type=MESH)

    lane = lax.broadcasted_iota(jnp.int32, (tb_size, 128), 1)

    def pair_tile(one, two):
        return jnp.where(lane == 0, one, jnp.where(lane == 1, two, 0.0))

    for part in range(2):
        own_load(0, part).wait()
    for o in range(half):
        x = xall[pl.ds(own_block(o) * tb_size, tb_size), :].astype(F32)
        st_own[o * tb_size:(o + 1) * tb_size, :] = pair_tile(
            jnp.sum(x, axis=1, keepdims=True), jnp.sum(x * x, axis=1, keepdims=True)
        )
    stats = st_own[...].T[0:8]
    st_tx[...] = stats
    st_rx[j] = stats
    square[...] = jnp.zeros_like(square)
    sq_tx[...] = jnp.zeros_like(sq_tx)
    pl.semaphore_wait(barrier, len(partners))

    def stat_copy(rel, d):
        target = at(y if rel == 0 else other, tr, z_peer(d))
        return remote(st_tx, st_rx.at[rel * nz + j], ss_sem, sr_sem.at[rel, d], target)

    stat_list = [(0, d) for d in range(1, nz)] + [(1, d) for d in range(nz)]
    for rel, d in stat_list:
        stat_copy(rel, d).start()
    for part in range(2):
        own_load(1, part).wait()

    def y_copy(which, o):
        ref = xall if which == 0 else call
        return remote(
            ref.at[pl.ds(own_block(o) * tb_size, tb_size)], ref.at[pl.ds((lead + o) * tb_size, tb_size)],
            ys_sem.at[which], yr_sem.at[which, o], at(other, tr, j),
        )

    for o in range(half):
        y_copy(1, o).start()
        y_copy(0, o).start()

    def statistics(rel):
        for d in range(1 if rel == 0 else 0, nz):
            source = lax.rem(j + nz - d, nz)
            remote(st_tx, st_rx.at[rel * nz + source], ss_sem, sr_sem.at[rel, d], here).wait_recv()
        total = st_rx[rel * nz]
        for z in range(1, nz):
            total = total + st_rx[rel * nz + z]
        total = total / width
        mean = total[0:1]
        flip[...] = jnp.zeros_like(flip)
        flip[0:1] = mean
        flip[1:2] = lax.rsqrt(total[1:2] - mean * mean + EPS)
        back = flip[...].T
        if rel == 0:
            ms[0:head] = back[0:head]
            ms[head + rows:] = back[head:]
        else:
            ms[head:head + rows] = back

    def xhat_of(t, span):
        tile = ms[block_rows(t), :]
        x = xall[block_rows(t), span].astype(F32)
        return x, (x - tile[:, 0:1]) * tile[:, 1:2]

    def is_far(t):
        return jnp.logical_and(t >= lead, t < lead + half)

    def normalize(t):
        @pl.when(t == 0)
        def _():
            statistics(0)

        @pl.when(t == lead)
        def _():
            statistics(1)

        for o in range(half):
            @pl.when(t == lead + o)
            def _(o=o):
                y_copy(1, o).wait_recv()
                y_copy(0, o).wait_recv()

        nall[block_rows(t), :] = xhat_of(t, slice(None))[1].astype(BF16)

    def to_mid(s):
        return remote(tx.at[s], rx.at[s], tx_sem, rx_sem.at[s], at(y, tr, inner))

    def across(s):
        return remote(tx.at[s], rm.at[s], tx_sem, rm_sem.at[s], at(y, tr, inner))

    def outward(s):
        span = hd.at[:, lax.rem(s, nfb), block_rows(s // nfb)]
        return remote(span, span, hs_sem, hr_sem.at[s], at(y, tr, outer))

    def partial_stage(s):
        t = s // nfb
        f = lax.rem(s, nfb)

        @pl.when(s < nfb)
        def _():
            wd_load(f).wait()
            wu_load(f).wait()

        @pl.when(f == 0)
        def _():
            normalize(t)

        parts = (
            contract(call[block_rows(t), :], wd[f], 1, 1),
            contract(nall[block_rows(t), :], wu[f], 1, 0),
        )

        @pl.when(is_end)
        def _():
            for k in range(2):
                tx[s, k] = parts[k].astype(BF16)
            to_mid(s).start()

        @pl.when(is_mid)
        def _():
            to_mid(s).wait_recv()
            for k in range(2):
                tx[s, k] = (parts[k] + rx[s, k].astype(F32)).astype(BF16)
            across(s).start()

    def act_stage(e):
        across(e).wait_recv()
        f = lax.rem(e, nfb)
        t = e // nfb

        def step(i, carry):
            r = pl.ds(pl.multiple_of(i * 16, 16), 16)
            out = pl.ds(pl.multiple_of(t * tb_size + i * 16, 16), 16)
            dhid = tx[e, 0, r, :].astype(F32) + rm[e, 0, r, :].astype(F32)
            pre = tx[e, 1, r, :].astype(F32) + rm[e, 1, r, :].astype(F32)
            phi = 0.5 * (1.0 + lax.erf(pre * SQRT_HALF))
            slope = phi + pre * jnp.exp(-0.5 * pre * pre) * INV_SQRT_2PI
            hd[0, f, out, :] = (pre * phi).astype(BF16)
            hd[1, f, out, :] = (dhid * slope).astype(BF16)
            return carry

        lax.fori_loop(0, tb_size // 16, step, 0)
        outward(e).start()

    def rs_copy(t, d):
        return remote(
            rs_tx.at[t, d - 1], rs_rx.at[t, d - 1], rss_sem, rsr_sem.at[t, d - 1],
            at(y, t_peer(d), j),
        )

    def columns(q):
        return pl.ds(pl.multiple_of(q * quarter, quarter), quarter)

    def use_stage(e):
        f = lax.rem(e, nfb)
        t = e // nfb

        @pl.when(is_end)
        def _():
            outward(e).wait_recv()

        @pl.when(f == 0)
        def _():
            acc[...] = jnp.zeros_like(acc)

        acc[0] += contract(hd[0, f, block_rows(t), :], wd[f], 1, 0)
        acc[1] += contract(hd[1, f, block_rows(t), :], wu[f], 1, 1)

        @pl.when(f == nfb - 1)
        def _():
            for d in range(1, nt):
                for k in range(2):
                    rs_tx[t, d - 1, k] = acc[k, :, columns(t_peer(d))].astype(BF16)
                rs_copy(t, d).start()
            for k in range(2):
                keep[t, k] = acc[k, :, columns(tr)]

    def first_rows(f, which):
        cols = pl.ds(pl.multiple_of(f * fb_size, fb_size), fb_size)
        if which == 0:
            grad_down[cols, :] = contract(hd[0, f, 0:rows, :], call[0:rows, :], 0, 0).astype(BF16)
        else:
            grad_up[:, cols] = contract(nall[0:rows, :], hd[1, f, 0:rows, :], 0, 0).astype(BF16)

    def last_rows(f, which):
        cols = pl.ds(pl.multiple_of(f * fb_size, fb_size), fb_size)
        if which == 0:
            part = contract(hd[0, f, rows:, :], call[rows:, :], 0, 0)
            grad_down[cols, :] = (grad_down[cols, :].astype(F32) + part).astype(BF16)
        else:
            part = contract(nall[rows:, :], hd[1, f, rows:, :], 0, 0)
            grad_up[:, cols] = (grad_up[:, cols].astype(F32) + part).astype(BF16)

    def yq_copy(o):
        return remote(y_tx.at[o], y_rx.at[o], yqs_sem, yqr_sem.at[o], at(other, tr, j))

    def ag_copy(o, d):
        return remote(
            ag_rx.at[o, tr], ag_rx.at[o, tr], ags_sem, agr_sem.at[o, d - 1],
            at(y, t_peer(d), j),
        )

    everyone = [(a, b) for a in range(nt) for b in range(nz) if a or b]

    def sq_copy(o, a, b):
        return remote(
            sq_tx.at[o], sq_rx.at[o, a * nz + b], sqs_sem, sqr_sem.at[o],
            at(y, t_peer(a), z_peer(b)),
        )

    def sq_all(o):
        span = sq_rx.at[o, pl.ds(1, nt * nz - 1)]
        return remote(span, span, sqs_sem, sqr_sem.at[o], here)

    def row_sum_stage(t):
        for d in range(1, nt):
            rs_copy(t, d).wait_recv()
        for k in range(2):
            total = keep[t, k]
            for d in range(1, nt):
                total = total + rs_rx[t, d - 1, k].astype(F32)
            keep[t, k] = total

        @pl.when(is_far(t))
        def _():
            for k in range(2):
                y_tx[t - lead, k] = keep[t, k].astype(BF16)
            yq_copy(t - lead).start()

    def gather_stage(o):
        t = jnp.where(o < lead, o, o + half)
        yq_copy(o).wait_recv()
        for k in range(2):
            ag_rx[o, tr, k] = (keep[t, k] + y_rx[o, k].astype(F32)).astype(BF16)
        for d in range(1, nt):
            ag_copy(o, d).start()
        dn = ag_rx[o, tr, 1].astype(F32)
        xhat = xhat_of(t, columns(tr))[1]
        square[0, 0:tb_size] = pair_tile(
            jnp.sum(dn, axis=1, keepdims=True), jnp.sum(dn * xhat, axis=1, keepdims=True)
        )
        sums = square[0].T[0:8]
        sq_tx[o] = sums
        sq_rx[o, 0] = sums
        for a, b in everyone:
            sq_copy(o, a, b).start()

    def finish_stage(o):
        t = jnp.where(o < lead, o, o + half)
        for d in range(1, nt):
            source = lax.rem(tr + nt - d, nt)
            remote(
                ag_rx.at[o, source], ag_rx.at[o, source], ags_sem,
                agr_sem.at[o, d - 1], here,
            ).wait_recv()
        sq_all(o).wait_recv()
        total = sq_rx[o, 0]
        for k in range(1, nt * nz):
            total = total + sq_rx[o, k]
        square[1, 0:8] = total / width
        means = square[1].T[0:tb_size]
        rstd = ms[block_rows(t), :][:, 1:2]
        for q in range(nt):
            span = slice(q * quarter, (q + 1) * quarter)
            x, xhat = xhat_of(t, span)
            mixed[block_rows(o), span] = (x + ag_rx[o, q, 0].astype(F32)).astype(BF16)
            dn = ag_rx[o, q, 1].astype(F32)
            grad[block_rows(o), span] = (
                call[block_rows(t), span].astype(F32)
                + rstd * (dn - means[:, 0:1] - xhat * means[:, 1:2])
            ).astype(BF16)

    pieces = 2 * nfb
    spread = nb // 2 // pieces

    def step(s, carry):
        @pl.when(s < nb)
        def _():
            with jax.named_scope("partial"):
                partial_stage(s)

        e = s - lag
        valid = jnp.logical_and(e >= 0, e < nb)

        @pl.when(jnp.logical_and(valid, is_mid))
        def _():
            with jax.named_scope("act"):
                act_stage(e)

        @pl.when(valid)
        def _():
            with jax.named_scope("use"):
                use_stage(e)

        g = e - nb // 2

        @pl.when(jnp.logical_and(g >= 0, jnp.logical_and(g < nb // 2, lax.rem(g, spread) == 0)))
        def _():
            with jax.named_scope("first"):
                p = g // spread

                @pl.when(p < nfb)
                def _():
                    first_rows(p, 0)

                @pl.when(p >= nfb)
                def _():
                    first_rows(p - nfb, 1)

        def done_block(shift, stage):
            k = e - shift - (nfb - 1)
            t = k // nfb

            @pl.when(jnp.logical_and(jnp.logical_and(k >= 0, t < ntb - 1), lax.rem(k, nfb) == 0))
            def _():
                stage(t)

        def gather_at(t):
            first = jnp.logical_and(t > lead, t <= half)

            @pl.when(jnp.logical_or(first, t >= half + lead))
            def _():
                with jax.named_scope("gather"):
                    gather_stage(jnp.where(first, t - lead - 1, t - half))

        done_block(ROW_SHIFT, row_sum_stage)
        done_block(ROW_SHIFT + 1, gather_at)
        return carry

    lax.fori_loop(0, nb + max(END_LAG, MID_LAG), step, 0)

    def last_piece(which):
        def body(f, carry):
            last_rows(f, which)
            return carry

        lax.fori_loop(0, nfb, body, 0)

    def finish_step(o, carry):
        finish_stage(o)
        return carry

    with jax.named_scope("last_down"):
        last_piece(0)
    with jax.named_scope("rowsum"):
        row_sum_stage(ntb - 1)
    with jax.named_scope("gather"):
        gather_stage(half - 1)
    with jax.named_scope("last_up"):
        last_piece(1)
    with jax.named_scope("finish"):
        lax.fori_loop(0, half, finish_step, 0)

    def sent(ref, sem):
        remote(ref, ref, sem, sem, here).wait_send()

    sent(st_rx.at[pl.ds(1, 2 * nz - 1)], ss_sem)
    far = pl.ds(head, rows)
    sent(xall.at[far], ys_sem.at[0])
    sent(call.at[far], ys_sem.at[1])
    sent(tx, tx_sem)

    @pl.when(is_mid)
    def _():
        sent(hd, hs_sem)

    sent(rs_tx, rss_sem)
    sent(y_tx, yqs_sem)
    sent(ag_rx.at[:, pl.ds(0, nt - 1)], ags_sem)
    sent(sq_rx.at[:, pl.ds(1, nt * nz - 1)], sqs_sem)


def line_call(nz, nt, tokens, w_up, w_down, cotangent):
    rows, depth = tokens.shape
    ff = w_up.shape[1]
    tb, fb = 64, FB_SIZE
    nfb = ff // fb
    ntb = 2 * rows // tb
    half = ntb // 2
    nb = nfb * ntb
    quarter = depth // nt
    vm = pltpu.VMEM
    dma = pltpu.SemaphoreType.DMA
    big = (nb, 2, tb, fb)
    scratch = [
        vm((2 * rows, depth), BF16), vm((2 * rows, depth), BF16), vm((2 * rows, depth), BF16),
        vm((nfb, depth, fb), BF16), vm((nfb, fb, depth), BF16),
        vm(big, BF16), vm(big, BF16), vm(big, BF16), vm((2, nfb, 2 * rows, fb), BF16),
        vm((rows, 128), F32), vm((8, rows), F32), vm((2 * nz, 8, rows), F32), vm((128, rows), F32),
        vm((2 * rows, 128), F32),
        vm((2, tb, depth), F32),
        vm((ntb, nt - 1, 2, tb, quarter), BF16), vm((ntb, nt - 1, 2, tb, quarter), BF16),
        vm((ntb, 2, tb, quarter), F32),
        vm((half, 2, tb, quarter), BF16), vm((half, 2, tb, quarter), BF16),
        vm((half, nt, 2, tb, quarter), BF16),
        vm((2, 128, 128), F32), vm((half, 8, 128), F32), vm((half, nt * nz, 8, 128), F32),
        dma((2, 2)), dma((nfb,)), dma((nfb,)),
        dma, dma((nb,)), dma((nb,)), dma, dma((nb,)),
        dma, dma((2, nz)), dma((2,)), dma((2, half)),
        dma, dma((ntb, nt - 1)), dma, dma((half,)),
        dma, dma((half, nt - 1)), dma, dma((half,)),
    ]
    return pl.pallas_call(
        functools.partial(line_kernel, (nz, nt, rows, depth, ff, tb, fb)),
        out_shape=tuple(
            OUT(shape, BF16)
            for shape in ((rows, depth), (rows, depth), (depth, ff), (ff, depth))
        ),
        in_specs=[pl.BlockSpec(memory_space=pl.ANY)] * 4,
        out_specs=[pl.BlockSpec(memory_space=pltpu.VMEM)] * 4,
        scratch_shapes=scratch,
        compiler_params=pltpu.CompilerParams(
            collective_id=0, has_side_effects=True, vmem_limit_bytes=VMEM_LIMIT
        ),
    )(tokens, w_up, w_down, cotangent)


def write_kernel(*refs):
    n = len(refs) // 2
    sems = refs[-1]
    copies = []
    for k in range(n):
        rows = refs[k].shape[0]
        cuts = 4 if rows * refs[k].shape[1] > 1 << 20 else 1
        for c in range(cuts):
            span = pl.ds(c * (rows // cuts), rows // cuts)
            copies.append((refs[k].at[span], refs[n + k].at[span]))
    copies = [pltpu.make_async_copy(a, b, sems.at[i]) for i, (a, b) in enumerate(copies)]
    for copy in copies:
        copy.start()
    for copy in copies:
        copy.wait()


def write_out(arrays):
    return pl.pallas_call(
        write_kernel,
        out_shape=tuple(jax.ShapeDtypeStruct(a.shape, a.dtype) for a in arrays),
        in_specs=[pl.BlockSpec(memory_space=pltpu.VMEM)] * len(arrays),
        out_specs=[pl.BlockSpec(memory_space=pl.ANY)] * len(arrays),
        scratch_shapes=[pltpu.SemaphoreType.DMA((16,))],
        compiler_params=pltpu.CompilerParams(vmem_limit_bytes=WRITE_LIMIT),
    )(*arrays)


def local_line(tokens, w_up, w_down, cotangent):
    nz = lax.axis_size("tcol")
    nt = lax.axis_size("trow")
    return write_out(line_call(nz, nt, tokens, w_up, w_down, cotangent))


def local_plain(tokens, w_up, w_down, cotangent):
    width = tokens.shape[1] * lax.axis_size("tcol")
    input_float = tokens.astype(F32)
    cot_all = lax.all_gather(cotangent, "fsdp", axis=0, tiled=True)
    sum_one, sum_two = lax.psum(
        (jnp.sum(input_float, axis=1), jnp.sum(input_float * input_float, axis=1)), "tcol"
    )
    token_mean = sum_one / width
    var = sum_two / width - token_mean * token_mean
    inverse_stddev = lax.rsqrt(var + EPS)
    centered_scaled = (input_float - token_mean[:, None]) * inverse_stddev[:, None]
    normalized_rows = centered_scaled.astype(BF16)
    normed_all = lax.all_gather(normalized_rows, "fsdp", axis=0, tiled=True)
    dhid_part = contract(cot_all, w_down, 1, 1).astype(BF16)
    dhid = lax.psum_scatter(dhid_part, "tcol", scatter_dimension=0, tiled=True).astype(F32)
    pre_part = contract(normed_all, w_up, 1, 0).astype(BF16)
    pre = lax.psum_scatter(pre_part, "tcol", scatter_dimension=0, tiled=True).astype(F32)
    hidden = lax.all_gather(gelu_value(pre).astype(BF16), "tcol", axis=0, tiled=True)
    dpre = lax.all_gather((dhid * gelu_slope(pre)).astype(BF16), "tcol", axis=0, tiled=True)
    branch_part = contract(hidden, w_down, 1, 0).astype(BF16)
    branch = lax.psum_scatter(branch_part, "fsdp", scatter_dimension=0, tiled=True)
    branch = lax.psum(branch, "trow").astype(F32)
    mixed = (input_float + branch).astype(BF16)
    grad_down = contract(hidden, cot_all, 0, 0).astype(BF16)
    dnorm_part = contract(dpre, w_up, 1, 1).astype(BF16)
    dnorm = lax.psum_scatter(dnorm_part, "fsdp", scatter_dimension=0, tiled=True)
    normed_gradient = lax.psum(dnorm, "trow").astype(F32)
    grad_up = contract(normed_all, dpre, 0, 0).astype(BF16)
    mean_first, mean_second = lax.psum(
        (jnp.sum(normed_gradient, axis=1), jnp.sum(normed_gradient * centered_scaled, axis=1)),
        "tcol",
    )
    first_moment = mean_first / width
    second_moment = mean_second / width
    input_gradient = cotangent.astype(F32) + inverse_stddev[:, None] * (
        normed_gradient - first_moment[:, None] - centered_scaled * second_moment[:, None]
    )
    return (mixed, input_gradient.astype(BF16), grad_up, grad_down)


def solution(mesh):
    fits = mesh.shape["fsdp"] == 2 and mesh.shape["tcol"] == 4
    return jax.shard_map(
        local_line if fits else local_plain,
        mesh=mesh,
        in_specs=(
            P("fsdp", "tcol"),
            P("tcol", ("fsdp", "trow")),
            P(("fsdp", "trow"), "tcol"),
            P("fsdp", "tcol"),
        ),
        out_specs=(
            P("fsdp", "tcol"),
            P("fsdp", "tcol"),
            P("tcol", ("fsdp", "trow")),
            P(("fsdp", "trow"), "tcol"),
        ),
        check_vma=False,
    )
```

```python
import functools

import jax
import jax.numpy as jnp
from jax import lax
from jax.experimental import pallas as pl
from jax.experimental.pallas import tpu as pltpu
from jax.sharding import PartitionSpec as P

MESH = pl.DeviceIdType.MESH
BF16 = jnp.bfloat16
F32 = jnp.float32
SQRT_HALF = 0.7071067811865476
INV_SQRT_2PI = 0.3989422804014327
EPS = 1e-05
END_LAG = 12
MID_LAG = 3
ROW_SHIFT = 5
RING = 15
MID_RING = 10
COLS_AT = 3
CUTS = 4
SUMS_AT = 1
FB_SIZE = 256
VMEM_LIMIT = 46 * 1024 * 1024
WRITE_LIMIT = 1024 * 1024
OUT = pltpu.VMEM


def gelu_value(pre):
    phi = 0.5 * (1.0 + jax.scipy.special.erf(pre * SQRT_HALF))
    return pre * phi


def gelu_slope(pre):
    phi = 0.5 * (1.0 + jax.scipy.special.erf(pre * SQRT_HALF))
    return phi + pre * jnp.exp(-0.5 * pre * pre) * INV_SQRT_2PI


def contract(left, right, left_dim, right_dim):
    return lax.dot_general(
        left, right, (((left_dim,), (right_dim,)), ((), ())), preferred_element_type=F32
    )


def line_kernel(
    sizes,
    tok_in, up_in, down_in, cot_in,
    mixed, grad, grad_up, grad_down,
    xall, call, nall, cs_tx, cs_rx, wu, wd, tx, rx, rm, hd,
    st_own, st_tx, st_rx, flip, ms, acc, rs_tx, rs_rx, keep, y_tx, y_rx, ag_rx, square, sq_tx, sq_rx,
    load_sem, wu_sem, wd_sem, tx_sem, rx_sem, rm_sem, hs_sem, hr_sem,
    ss_sem, sr_sem, ys_sem, yr_sem, rss_sem, rsr_sem, yqs_sem, yqr_sem, ags_sem, agr_sem,
    sqs_sem, sqr_sem, css_sem, csr_sem,
):
    nz, nt, rows, depth, ff, tb_size, fb_size = sizes
    nfb = ff // fb_size
    ntb = 2 * rows // tb_size
    half = ntb // 2
    lead = half // 2
    nb = ntb * nfb
    quarter = depth // nt
    width = depth * nz
    y = lax.axis_index("fsdp")
    tr = lax.axis_index("trow")
    j = lax.axis_index("tcol")
    mid_low = nz // 2 - 1
    is_mid = jnp.logical_or(j == mid_low, j == mid_low + 1)
    is_end = jnp.logical_not(is_mid)
    is_odd = lax.rem(tr, 2) == 1
    inner = jnp.where(j <= mid_low, j + 1, j - 1)
    outer = jnp.where(j <= mid_low, jnp.maximum(j - 1, 0), jnp.minimum(j + 1, nz - 1))
    lag = jnp.where(is_mid, MID_LAG, END_LAG)
    other = 1 - y

    def at(yy, tt, jj):
        return {"fsdp": yy, "trow": tt, "tcol": jj}

    def remote(src, dst, send, recv, device):
        return pltpu.make_async_remote_copy(
            src_ref=src, dst_ref=dst, send_sem=send, recv_sem=recv,
            device_id=device, device_id_type=MESH,
        )

    def z_peer(d):
        return lax.rem(j + d, nz)

    def t_peer(d):
        return lax.rem(tr + d, nt)

    here = at(y, tr, j)

    def own_block(o):
        return o if o < lead else o + half

    def block_rows(t):
        return pl.ds(pl.multiple_of(t * tb_size, tb_size), tb_size)

    head = lead * tb_size
    spans = [(pl.ds(0, head), pl.ds(0, head)), (pl.ds(head, rows - head), pl.ds(head + rows, rows - head))]

    def own_load(which, part):
        source, dest = (tok_in, xall) if which == 0 else (cot_in, call)
        return pltpu.make_async_copy(
            source.at[spans[part][0]], dest.at[spans[part][1]], load_sem.at[which, part]
        )

    def wd_load(f):
        return pltpu.make_async_copy(
            down_in.at[pl.ds(pl.multiple_of(f * fb_size, fb_size), fb_size)], wd.at[f], wd_sem.at[f]
        )

    def wu_load(f):
        return pltpu.make_async_copy(
            up_in.at[:, pl.ds(pl.multiple_of(f * fb_size, fb_size), fb_size)], wu.at[f], wu_sem.at[f]
        )

    own_load(1, 0).start()
    own_load(0, 0).start()
    wd_load(0).start()
    wu_load(0).start()

    barrier = pltpu.get_barrier_semaphore()
    partners = [(y, t_peer(a), z_peer(b)) for a in range(nt) for b in range(nz) if a or b]
    partners += [(other, tr, z_peer(b)) for b in range(nz)]
    for device in partners:
        pl.semaphore_signal(barrier, inc=1, device_id=at(*device), device_id_type=MESH)

    lane = lax.broadcasted_iota(jnp.int32, (tb_size, 128), 1)

    def pair_tile(one, two):
        return jnp.where(lane == 0, one, jnp.where(lane == 1, two, 0.0))

    own_load(0, 1).start()
    for f in range(1, nfb):
        wu_load(f).start()
        wd_load(f).start()
    own_load(1, 1).start()
    square[...] = jnp.zeros_like(square)
    sq_tx[...] = jnp.zeros_like(sq_tx)
    own_load(1, 0).wait()
    own_load(0, 0).wait()

    x = xall[0:tb_size, :].astype(F32)
    nall[0:tb_size, :] = (x - jnp.sum(x, axis=1, keepdims=True) / depth).astype(BF16)

    def parts_of(t, f):
        return (
            contract(call[block_rows(t), :], wd[f], 1, 1),
            contract(nall[block_rows(t), :], wu[f], 1, 0),
        )

    def to_mid(s):
        return remote(tx.at[s], rx.at[s], tx_sem, rx_sem.at[lax.rem(s, RING)], at(y, tr, inner))

    @pl.when(is_end)
    def _():
        wd_load(0).wait()
        wu_load(0).wait()
        parts = parts_of(0, 0)
        for k in range(2):
            tx[0, k] = parts[k].astype(BF16)

    pl.semaphore_wait(barrier, len(partners))

    @pl.when(is_end)
    def _():
        to_mid(0).start()

    def stat_copy(rel, d):
        target = at(y if rel == 0 else other, tr, z_peer(d))
        return remote(st_tx, st_rx.at[rel * nz + j], ss_sem, sr_sem.at[rel], target)

    stat_list = [(0, d) for d in range(1, nz)] + [(1, d) for d in range(nz)]

    def y_copy(which, o):
        ref = xall if which == 0 else call
        return remote(
            ref.at[pl.ds(own_block(o) * tb_size, tb_size)], ref.at[pl.ds((lead + o) * tb_size, tb_size)],
            ys_sem.at[which], yr_sem.at[which, o], at(other, tr, j),
        )

    def cs_copy(z):
        return remote(cs_tx, cs_rx.at[j], css_sem, csr_sem, at(y, tr, z))

    mids = (mid_low, mid_low + 1)

    def token_sums():
        own_load(0, 1).wait()
        for o in range(half):
            x = xall[pl.ds(own_block(o) * tb_size, tb_size), :].astype(F32)
            st_own[o * tb_size:(o + 1) * tb_size, :] = pair_tile(
                jnp.sum(x, axis=1, keepdims=True), jnp.sum(x * x, axis=1, keepdims=True)
            )
        stats = st_own[...].T[0:2]
        st_tx[...] = stats
        st_rx[j] = stats
        for rel, d in stat_list:
            if rel == 0:
                stat_copy(rel, d).start()

    def column_sums(waited):
        ones = jnp.ones((8, depth), BF16)
        for f in range(nfb):
            if f >= waited:
                wu_load(f).wait()
            cs_tx[f:f + 1] = contract(ones, wu[f], 1, 0)[0:1]
        for z in mids:
            @pl.when(j != z)
            def _(z=z):
                cs_copy(z).start()

        @pl.when(is_mid)
        def _():
            cs_rx[j] = cs_tx[...]

        for rel, d in stat_list:
            if rel == 1:
                stat_copy(rel, d).start()
        own_load(1, 1).wait()
        for o in range(half):
            y_copy(1, o).start()
            y_copy(0, o).start()

    def statistics(rel):
        span = st_rx.at[pl.ds(rel * nz, nz - 1 + rel)]
        remote(span, span, ss_sem, sr_sem.at[rel], here).wait_recv()
        total = st_rx[rel * nz]
        for z in range(1, nz):
            total = total + st_rx[rel * nz + z]
        total = total / width
        mean = total[0:1]
        flip[...] = jnp.zeros_like(flip)
        flip[0:1] = mean
        rstd = lax.rsqrt(total[1:2] - mean * mean + EPS)
        flip[1:2] = rstd
        for z in range(nz):
            flip[2 + z:3 + z] = rstd * (st_rx[rel * nz + z][0:1] / depth - mean)
        back = flip[...].T
        if rel == 0:
            ms[0:head] = back[0:head]
            ms[head + rows:] = back[head:]
        else:
            ms[head:head + rows] = back

    def xhat_of(t, span):
        tile = ms[block_rows(t), :]
        x = xall[block_rows(t), span].astype(F32)
        return x, (x - tile[:, 0:1]) * tile[:, 1:2]

    def is_far(t):
        return jnp.logical_and(t >= lead, t < lead + half)

    def norm_rows(t):
        nall[block_rows(t), :] = xhat_of(t, slice(None))[1].astype(BF16)

    def first_statistics():
        statistics(0)

        @pl.when(is_mid)
        def _():
            span = cs_rx.at[pl.ds(0, nz - 1)]
            remote(span, span, css_sem, csr_sem, here).wait_recv()

    def make_rows(t):
        @pl.when(t == 1)
        def _():
            norm_rows(0)

        @pl.when(t == lead)
        def _():
            statistics(1)

        for o in range(half):
            @pl.when(t == lead + o)
            def _(o=o):
                y_copy(1, o).wait_recv()
                y_copy(0, o).wait_recv()

        @pl.when(t > 0)
        def _():
            norm_rows(t)

    def across(s):
        return remote(tx.at[s], rm.at[s], tx_sem, rm_sem.at[lax.rem(s, MID_RING)], at(y, tr, inner))

    def outward(s):
        span = hd.at[:, lax.rem(s, nfb), block_rows(s // nfb)]
        return remote(span, span, hs_sem, hr_sem.at[lax.rem(s, RING)], at(y, tr, outer))

    def partial_stage(s):
        t = s // nfb
        f = lax.rem(s, nfb)

        @pl.when(s < nfb)
        def _():
            wd_load(f).wait()

        @pl.when(f == 0)
        def _():
            make_rows(t)

        parts = parts_of(t, f)

        @pl.when(is_end)
        def _():
            for k in range(2):
                tx[s, k] = parts[k].astype(BF16)
            to_mid(s).start()

        @pl.when(is_mid)
        def _():
            to_mid(s).wait_recv()
            for k in range(2):
                tx[s, k] = (parts[k] + rx[s, k].astype(F32)).astype(BF16)
            across(s).start()

    def act_stage(e):
        across(e).wait_recv()
        f = lax.rem(e, nfb)
        t = e // nfb

        def step(first, i, carry):
            r = pl.ds(pl.multiple_of(i * 16, 16), 16)
            out = pl.ds(pl.multiple_of(t * tb_size + i * 16, 16), 16)
            dhid = tx[e, 0, r, :].astype(F32) + rm[e, 0, r, :].astype(F32)
            pre = tx[e, 1, r, :].astype(F32) + rm[e, 1, r, :].astype(F32)
            if first:
                tile = ms[out, :]
                pre = pre * tile[:, 1:2]
                for z in range(nz):
                    pre = pre + tile[:, 2 + z:3 + z] * cs_rx[z, pl.ds(f, 1), :]
            phi = 0.5 * (1.0 + lax.erf(pre * SQRT_HALF))
            slope = phi + pre * jnp.exp(-0.5 * pre * pre) * INV_SQRT_2PI
            hd[0, f, out, :] = (pre * phi).astype(BF16)
            hd[1, f, out, :] = (dhid * slope).astype(BF16)
            return carry

        for first in (True, False):
            @pl.when((e < nfb) == first)
            def _(first=first):
                lax.fori_loop(0, tb_size // 16, functools.partial(step, first), 0)

        outward(e).start()

    def rs_copy(t, d, k):
        return remote(
            rs_tx.at[t, d - 1, k], rs_rx.at[t, d - 1, k], rss_sem, rsr_sem.at[t],
            at(y, t_peer(d), j),
        )

    def columns(q):
        return pl.ds(pl.multiple_of(q * quarter, quarter), quarter)

    def use_stage(e):
        f = lax.rem(e, nfb)
        t = e // nfb

        @pl.when(is_end)
        def _():
            outward(e).wait_recv()

        @pl.when(f == 0)
        def _():
            acc[...] = jnp.zeros_like(acc)

        def summed(k):
            @pl.when(f == nfb - 1)
            def _():
                for d in range(1, nt):
                    rs_tx[t, d - 1, k] = acc[k, :, columns(t_peer(d))].astype(BF16)
                    rs_copy(t, d, k).start()
                keep[t, k] = acc[k, :, columns(tr)]

        acc[0] += contract(hd[0, f, block_rows(t), :], wd[f], 1, 0)
        acc[1] += contract(hd[1, f, block_rows(t), :], wu[f], 1, 1)
        summed(0)
        summed(1)

    def first_rows(f, which):
        cols = pl.ds(pl.multiple_of(f * fb_size, fb_size), fb_size)
        if which == 0:
            grad_down[cols, :] = contract(hd[0, f, 0:rows, :], call[0:rows, :], 0, 0).astype(BF16)
        else:
            grad_up[:, cols] = contract(nall[0:rows, :], hd[1, f, 0:rows, :], 0, 0).astype(BF16)

    def last_rows(f, which):
        cols = pl.ds(pl.multiple_of(f * fb_size, fb_size), fb_size)
        if which == 0:
            part = contract(hd[0, f, rows:, :], call[rows:, :], 0, 0)
            grad_down[cols, :] = (grad_down[cols, :].astype(F32) + part).astype(BF16)
        else:
            part = contract(nall[rows:, :], hd[1, f, rows:, :], 0, 0)
            grad_up[:, cols] = (grad_up[:, cols].astype(F32) + part).astype(BF16)

    def yq_copy(o):
        return remote(y_tx.at[o], y_rx.at[o], yqs_sem, yqr_sem.at[o], at(other, tr, j))

    def ag_copy(o, d, k):
        return remote(
            ag_rx.at[o, tr, k], ag_rx.at[o, tr, k], ags_sem, agr_sem.at[o],
            at(y, t_peer(d), j),
        )

    everyone = [(a, b) for a in range(nt) for b in range(nz) if a or b]

    def sq_copy(o, a, b):
        return remote(
            sq_tx.at[o], sq_rx.at[o, a * nz + b], sqs_sem, sqr_sem.at[o],
            at(y, t_peer(a), z_peer(b)),
        )

    def sq_all(o):
        span = sq_rx.at[o, pl.ds(1, nt * nz - 1)]
        return remote(span, span, sqs_sem, sqr_sem.at[o], here)

    def row_sum_stage(t):
        remote(rs_tx.at[t], rs_rx.at[t], rss_sem, rsr_sem.at[t], here).wait_recv()
        for k in range(2):
            total = keep[t, k]
            for d in range(1, nt):
                total = total + rs_rx[t, d - 1, k].astype(F32)
            keep[t, k] = total

        @pl.when(is_far(t))
        def _():
            for k in range(2):
                y_tx[t - lead, k] = keep[t, k].astype(BF16)
            yq_copy(t - lead).start()

    def gather_stage(o):
        t = jnp.where(o < lead, o, o + half)
        yq_copy(o).wait_recv()
        for k in range(2):
            ag_rx[o, tr, k] = (keep[t, k] + y_rx[o, k].astype(F32)).astype(BF16)
            if k == 0:
                for d in range(1, nt):
                    ag_copy(o, d, k).start()
        dn = ag_rx[o, tr, 1].astype(F32)
        xhat = xhat_of(t, columns(tr))[1]
        square[0, 0:tb_size] = pair_tile(
            jnp.sum(dn, axis=1, keepdims=True), jnp.sum(dn * xhat, axis=1, keepdims=True)
        )
        sums = square[0].T[0:2]
        sq_tx[o] = sums
        sq_rx[o, 0] = sums
        for a, b in everyone:
            sq_copy(o, a, b).start()
        for d in range(1, nt):
            ag_copy(o, d, 1).start()

    def finish_stage(o):
        t = jnp.where(o < lead, o, o + half)
        span = ag_rx.at[o, pl.ds(0, nt - 1)]
        remote(span, span, ags_sem, agr_sem.at[o], here).wait_recv()
        sq_all(o).wait_recv()
        total = sq_rx[o, 0]
        for k in range(1, nt * nz):
            total = total + sq_rx[o, k]
        square[1, 0:2] = total / width
        means = square[1].T[0:tb_size]
        rstd = ms[block_rows(t), :][:, 1:2]
        for q in range(nt):
            span = slice(q * quarter, (q + 1) * quarter)
            x, xhat = xhat_of(t, span)
            mixed[block_rows(o), span] = (x + ag_rx[o, q, 0].astype(F32)).astype(BF16)
            dn = ag_rx[o, q, 1].astype(F32)
            grad[block_rows(o), span] = (
                call[block_rows(t), span].astype(F32)
                + rstd * (dn - means[:, 0:1] - xhat * means[:, 1:2])
            ).astype(BF16)

    pieces = 2 * nfb
    spread = nb // 2 // pieces

    def step(s, carry):
        @pl.when(jnp.logical_and(s == 0, jnp.logical_or(is_mid, is_odd)))
        def _():
            with jax.named_scope("sums"):
                token_sums()

        @pl.when(jnp.logical_and(s == 0, is_mid))
        def _():
            with jax.named_scope("cols"):
                column_sums(0)

        @pl.when(jnp.logical_and(jnp.logical_and(s > 0, s <= COLS_AT), is_end))
        def _():
            wu_load(s).wait()

        @pl.when(jnp.logical_and(s == nfb, is_end))
        def _():
            with jax.named_scope("norm"):
                first_statistics()

        @pl.when(jnp.logical_and(s < nb, jnp.logical_or(is_mid, s > 0)))
        def _():
            with jax.named_scope("partial"):
                partial_stage(s)

        @pl.when(jnp.logical_and(s == SUMS_AT, jnp.logical_and(is_end, jnp.logical_not(is_odd))))
        def _():
            with jax.named_scope("sums"):
                token_sums()

        @pl.when(jnp.logical_and(s == COLS_AT, is_end))
        def _():
            with jax.named_scope("cols"):
                column_sums(COLS_AT + 1)

        e = s - lag
        valid = jnp.logical_and(e >= 0, e < nb)

        @pl.when(jnp.logical_and(e == 0, is_mid))
        def _():
            with jax.named_scope("norm"):
                first_statistics()

        @pl.when(jnp.logical_and(valid, is_mid))
        def _():
            with jax.named_scope("act"):
                act_stage(e)

        @pl.when(valid)
        def _():
            with jax.named_scope("use"):
                use_stage(e)

        g = e - nb // 2

        @pl.when(jnp.logical_and(g >= 0, jnp.logical_and(g < nb // 2, lax.rem(g, spread) == 0)))
        def _():
            with jax.named_scope("first"):
                p = g // spread

                @pl.when(p < nfb)
                def _():
                    first_rows(p, 0)

                @pl.when(p >= nfb)
                def _():
                    first_rows(p - nfb, 1)

        def done_block(shift, stage):
            k = e - shift - (nfb - 1)
            t = k // nfb

            @pl.when(jnp.logical_and(jnp.logical_and(k >= 0, t < ntb - 1), lax.rem(k, nfb) == 0))
            def _():
                stage(t)

        def gather_at(t):
            first = jnp.logical_and(t > lead, t <= half)

            @pl.when(jnp.logical_or(first, t >= half + lead))
            def _():
                with jax.named_scope("gather"):
                    gather_stage(jnp.where(first, t - lead - 1, t - half))

        done_block(ROW_SHIFT, row_sum_stage)
        done_block(ROW_SHIFT + 1, gather_at)
        return carry

    lax.fori_loop(0, nb + max(END_LAG, MID_LAG), step, 0)

    def last_piece(which):
        def body(f, carry):
            last_rows(f, which)
            return carry

        lax.fori_loop(0, nfb, body, 0)

    def finish_step(o, carry):
        finish_stage(o)
        return carry

    with jax.named_scope("last_down"):
        last_piece(0)
    with jax.named_scope("rowsum"):
        row_sum_stage(ntb - 1)
    with jax.named_scope("gather"):
        gather_stage(half - 1)
    with jax.named_scope("last_up"):
        last_piece(1)
    with jax.named_scope("finish"):
        lax.fori_loop(0, half, finish_step, 0)

    def sent(ref, sem):
        remote(ref, ref, sem, sem, here).wait_send()

    with jax.named_scope("drain"):
        sent(st_rx.at[pl.ds(1, 2 * nz - 1)], ss_sem)
    far = pl.ds(head, rows)
    sent(xall.at[far], ys_sem.at[0])
    sent(call.at[far], ys_sem.at[1])
    sent(tx, tx_sem)

    @pl.when(is_end)
    def _():
        sent(cs_rx.at[pl.ds(0, 2)], css_sem)

    @pl.when(is_mid)
    def _():
        sent(cs_rx.at[0], css_sem)


    @pl.when(is_mid)
    def _():
        sent(hd, hs_sem)

    sent(rs_tx, rss_sem)
    sent(y_tx, yqs_sem)
    sent(ag_rx.at[:, pl.ds(0, nt - 1)], ags_sem)
    sent(sq_rx.at[:, pl.ds(1, nt * nz - 1)], sqs_sem)


def line_call(nz, nt, tokens, w_up, w_down, cotangent):
    rows, depth = tokens.shape
    ff = w_up.shape[1]
    tb, fb = 64, FB_SIZE
    nfb = ff // fb
    ntb = 2 * rows // tb
    half = ntb // 2
    nb = nfb * ntb
    quarter = depth // nt
    sums = -(-nfb // 8) * 8
    vm = pltpu.VMEM
    dma = pltpu.SemaphoreType.DMA
    big = (nb, 2, tb, fb)
    scratch = [
        vm((2 * rows, depth), BF16), vm((2 * rows, depth), BF16), vm((2 * rows, depth), BF16),
        vm((sums, fb), F32), vm((nz, sums, fb), F32),
        vm((nfb, depth, fb), BF16), vm((nfb, fb, depth), BF16),
        vm(big, BF16), vm(big, BF16), vm(big, BF16), vm((2, nfb, 2 * rows, fb), BF16),
        vm((rows, 128), F32), vm((2, rows), F32), vm((2 * nz, 2, rows), F32), vm((128, rows), F32),
        vm((2 * rows, 128), F32),
        vm((2, tb, depth), F32),
        vm((ntb, nt - 1, 2, tb, quarter), BF16), vm((ntb, nt - 1, 2, tb, quarter), BF16),
        vm((ntb, 2, tb, quarter), F32),
        vm((half, 2, tb, quarter), BF16), vm((half, 2, tb, quarter), BF16),
        vm((half, nt, 2, tb, quarter), BF16),
        vm((2, 128, 128), F32), vm((half, 2, 128), F32), vm((half, nt * nz, 2, 128), F32),
        dma((2, 2)), dma((nfb,)), dma((nfb,)),
        dma, dma((RING,)), dma((MID_RING,)), dma, dma((RING,)),
        dma, dma((2,)), dma((2,)), dma((2, half)),
        dma, dma((ntb,)), dma, dma((half,)),
        dma, dma((half,)), dma, dma((half,)), dma, dma,
    ]
    return pl.pallas_call(
        functools.partial(line_kernel, (nz, nt, rows, depth, ff, tb, fb)),
        out_shape=tuple(
            OUT(shape, BF16)
            for shape in ((rows, depth), (rows, depth), (depth, ff), (ff, depth))
        ),
        in_specs=[pl.BlockSpec(memory_space=pl.ANY)] * 4,
        out_specs=[pl.BlockSpec(memory_space=pltpu.VMEM)] * 4,
        scratch_shapes=scratch,
        compiler_params=pltpu.CompilerParams(
            collective_id=0, has_side_effects=True, vmem_limit_bytes=VMEM_LIMIT
        ),
    )(tokens, w_up, w_down, cotangent)


def write_kernel(*refs):
    n = len(refs) // 2
    sems = refs[-1]
    copies = []
    for k in range(n):
        rows = refs[k].shape[0]
        cuts = CUTS if rows * refs[k].shape[1] > 1 << 20 else 1
        for c in range(cuts):
            span = pl.ds(c * (rows // cuts), rows // cuts)
            copies.append((refs[k].at[span], refs[n + k].at[span]))
    copies = [pltpu.make_async_copy(a, b, sems.at[i]) for i, (a, b) in enumerate(copies)]
    for copy in copies:
        copy.start()
    for copy in copies:
        copy.wait()


def write_out(arrays):
    return pl.pallas_call(
        write_kernel,
        out_shape=tuple(jax.ShapeDtypeStruct(a.shape, a.dtype) for a in arrays),
        in_specs=[pl.BlockSpec(memory_space=pltpu.VMEM)] * len(arrays),
        out_specs=[pl.BlockSpec(memory_space=pl.ANY)] * len(arrays),
        scratch_shapes=[pltpu.SemaphoreType.DMA((4 * CUTS,))],
        compiler_params=pltpu.CompilerParams(vmem_limit_bytes=WRITE_LIMIT),
    )(*arrays)


def local_line(tokens, w_up, w_down, cotangent):
    nz = lax.axis_size("tcol")
    nt = lax.axis_size("trow")
    return write_out(line_call(nz, nt, tokens, w_up, w_down, cotangent))


def local_plain(tokens, w_up, w_down, cotangent):
    width = tokens.shape[1] * lax.axis_size("tcol")
    input_float = tokens.astype(F32)
    cot_all = lax.all_gather(cotangent, "fsdp", axis=0, tiled=True)
    sum_one, sum_two = lax.psum(
        (jnp.sum(input_float, axis=1), jnp.sum(input_float * input_float, axis=1)), "tcol"
    )
    token_mean = sum_one / width
    var = sum_two / width - token_mean * token_mean
    inverse_stddev = lax.rsqrt(var + EPS)
    centered_scaled = (input_float - token_mean[:, None]) * inverse_stddev[:, None]
    normalized_rows = centered_scaled.astype(BF16)
    normed_all = lax.all_gather(normalized_rows, "fsdp", axis=0, tiled=True)
    dhid_part = contract(cot_all, w_down, 1, 1).astype(BF16)
    dhid = lax.psum_scatter(dhid_part, "tcol", scatter_dimension=0, tiled=True).astype(F32)
    pre_part = contract(normed_all, w_up, 1, 0).astype(BF16)
    pre = lax.psum_scatter(pre_part, "tcol", scatter_dimension=0, tiled=True).astype(F32)
    hidden = lax.all_gather(gelu_value(pre).astype(BF16), "tcol", axis=0, tiled=True)
    dpre = lax.all_gather((dhid * gelu_slope(pre)).astype(BF16), "tcol", axis=0, tiled=True)
    branch_part = contract(hidden, w_down, 1, 0).astype(BF16)
    branch = lax.psum_scatter(branch_part, "fsdp", scatter_dimension=0, tiled=True)
    branch = lax.psum(branch, "trow").astype(F32)
    mixed = (input_float + branch).astype(BF16)
    grad_down = contract(hidden, cot_all, 0, 0).astype(BF16)
    dnorm_part = contract(dpre, w_up, 1, 1).astype(BF16)
    dnorm = lax.psum_scatter(dnorm_part, "fsdp", scatter_dimension=0, tiled=True)
    normed_gradient = lax.psum(dnorm, "trow").astype(F32)
    grad_up = contract(normed_all, dpre, 0, 0).astype(BF16)
    mean_first, mean_second = lax.psum(
        (jnp.sum(normed_gradient, axis=1), jnp.sum(normed_gradient * centered_scaled, axis=1)),
        "tcol",
    )
    first_moment = mean_first / width
    second_moment = mean_second / width
    input_gradient = cotangent.astype(F32) + inverse_stddev[:, None] * (
        normed_gradient - first_moment[:, None] - centered_scaled * second_moment[:, None]
    )
    return (mixed, input_gradient.astype(BF16), grad_up, grad_down)


def solution(mesh):
    fits = mesh.shape["fsdp"] == 2 and mesh.shape["tcol"] == 4
    return jax.shard_map(
        local_line if fits else local_plain,
        mesh=mesh,
        in_specs=(
            P("fsdp", "tcol"),
            P("tcol", ("fsdp", "trow")),
            P(("fsdp", "trow"), "tcol"),
            P("fsdp", "tcol"),
        ),
        out_specs=(
            P("fsdp", "tcol"),
            P("fsdp", "tcol"),
            P("tcol", ("fsdp", "trow")),
            P(("fsdp", "trow"), "tcol"),
        ),
        check_vma=False,
    )
```

```python
import functools

import jax
import jax.numpy as jnp
from jax import lax
from jax.experimental import pallas as pl
from jax.experimental.pallas import tpu as pltpu
from jax.sharding import PartitionSpec as P

MESH = pl.DeviceIdType.MESH
BF16 = jnp.bfloat16
F32 = jnp.float32
SQRT_HALF = 0.7071067811865476
INV_SQRT_2PI = 0.3989422804014327
EPS = 1e-05
END_LAG = 12
MID_LAG = 3
ROW_SHIFT = 5
RING = 15
MID_RING = 10
COLS_AT = 3
CUTS = 4
SUMS_AT = 1
FB_SIZE = 256
VMEM_LIMIT = 46 * 1024 * 1024
WRITE_LIMIT = 1024 * 1024
OUT = pltpu.VMEM


def gelu_value(pre):
    phi = 0.5 * (1.0 + jax.scipy.special.erf(pre * SQRT_HALF))
    return pre * phi


def gelu_slope(pre):
    phi = 0.5 * (1.0 + jax.scipy.special.erf(pre * SQRT_HALF))
    return phi + pre * jnp.exp(-0.5 * pre * pre) * INV_SQRT_2PI


def contract(left, right, left_dim, right_dim):
    return lax.dot_general(
        left, right, (((left_dim,), (right_dim,)), ((), ())), preferred_element_type=F32
    )


def line_kernel(
    sizes,
    tok_in, up_in, down_in, cot_in,
    mixed, grad, grad_up, grad_down,
    xall, call, nall, cs_tx, cs_rx, wu, wd, tx, rx, rm, hd,
    st_own, st_tx, st_rx, flip, ms, acc, pr_tx, pr_rx, keep, y_tx, y_rx, cr_tx, cr_rx, fin, square, sq_tx, sq_rx, fm_rx,
    load_sem, wu_sem, wd_sem, tx_sem, rx_sem, rm_sem, hs_sem, hr_sem,
    ss_sem, sr_sem, ys_sem, yr_sem, prs_sem, prr_sem, yqs_sem, yqr_sem, crs_sem, crr_sem, fis_sem, fir_sem,
    sqs_sem, sqr_sem, css_sem, csr_sem, fms_sem, fmr_sem,
):
    nz, nt, rows, depth, ff, tb_size, fb_size = sizes
    nfb = ff // fb_size
    ntb = 2 * rows // tb_size
    half = ntb // 2
    lead = half // 2
    nb = ntb * nfb
    side = depth // 2
    width = depth * nz
    y = lax.axis_index("fsdp")
    tr = lax.axis_index("trow")
    j = lax.axis_index("tcol")
    mid_low = nz // 2 - 1
    is_mid = jnp.logical_or(j == mid_low, j == mid_low + 1)
    is_end = jnp.logical_not(is_mid)
    core = lax.rem(tr, 2)
    is_odd = core == 1
    pair = tr + 1 - 2 * core
    cross = lax.rem(tr + nt // 2, nt)
    inner = jnp.where(j <= mid_low, j + 1, j - 1)
    outer = jnp.where(j <= mid_low, jnp.maximum(j - 1, 0), jnp.minimum(j + 1, nz - 1))
    lag = jnp.where(is_mid, MID_LAG, END_LAG)
    other = 1 - y

    def at(yy, tt, jj):
        return {"fsdp": yy, "trow": tt, "tcol": jj}

    def remote(src, dst, send, recv, device):
        return pltpu.make_async_remote_copy(
            src_ref=src, dst_ref=dst, send_sem=send, recv_sem=recv,
            device_id=device, device_id_type=MESH,
        )

    def z_peer(d):
        return lax.rem(j + d, nz)

    def t_peer(d):
        return lax.rem(tr + d, nt)

    here = at(y, tr, j)

    def own_block(o):
        return o if o < lead else o + half

    def block_rows(t):
        return pl.ds(pl.multiple_of(t * tb_size, tb_size), tb_size)

    head = lead * tb_size
    spans = [(pl.ds(0, head), pl.ds(0, head)), (pl.ds(head, rows - head), pl.ds(head + rows, rows - head))]

    def own_load(which, part):
        source, dest = (tok_in, xall) if which == 0 else (cot_in, call)
        return pltpu.make_async_copy(
            source.at[spans[part][0]], dest.at[spans[part][1]], load_sem.at[which, part]
        )

    def wd_load(f):
        return pltpu.make_async_copy(
            down_in.at[pl.ds(pl.multiple_of(f * fb_size, fb_size), fb_size)], wd.at[f], wd_sem.at[f]
        )

    def wu_load(f):
        return pltpu.make_async_copy(
            up_in.at[:, pl.ds(pl.multiple_of(f * fb_size, fb_size), fb_size)], wu.at[f], wu_sem.at[f]
        )

    own_load(1, 0).start()
    own_load(0, 0).start()
    wd_load(0).start()
    wu_load(0).start()

    barrier = pltpu.get_barrier_semaphore()
    partners = [(y, t_peer(a), z_peer(b)) for a in range(nt) for b in range(nz) if a or b]
    partners += [(other, tr, z_peer(b)) for b in range(nz)]
    for device in partners:
        pl.semaphore_signal(barrier, inc=1, device_id=at(*device), device_id_type=MESH)

    lane = lax.broadcasted_iota(jnp.int32, (tb_size, 128), 1)

    def pair_tile(one, two):
        return jnp.where(lane == 0, one, jnp.where(lane == 1, two, 0.0))

    own_load(0, 1).start()
    for f in range(1, nfb):
        wu_load(f).start()
        wd_load(f).start()
    own_load(1, 1).start()
    square[...] = jnp.zeros_like(square)
    sq_tx[...] = jnp.zeros_like(sq_tx)
    own_load(1, 0).wait()
    own_load(0, 0).wait()

    x = xall[0:tb_size, :].astype(F32)
    nall[0:tb_size, :] = (x - jnp.sum(x, axis=1, keepdims=True) / depth).astype(BF16)

    def parts_of(t, f):
        return (
            contract(call[block_rows(t), :], wd[f], 1, 1),
            contract(nall[block_rows(t), :], wu[f], 1, 0),
        )

    def to_mid(s):
        return remote(tx.at[s], rx.at[s], tx_sem, rx_sem.at[lax.rem(s, RING)], at(y, tr, inner))

    @pl.when(is_end)
    def _():
        wd_load(0).wait()
        wu_load(0).wait()
        parts = parts_of(0, 0)
        for k in range(2):
            tx[0, k] = parts[k].astype(BF16)

    pl.semaphore_wait(barrier, len(partners))

    @pl.when(is_end)
    def _():
        to_mid(0).start()

    def stat_copy(rel, d):
        target = at(y if rel == 0 else other, tr, z_peer(d))
        return remote(st_tx, st_rx.at[rel * nz + j], ss_sem, sr_sem.at[rel], target)

    stat_list = [(0, d) for d in range(1, nz)] + [(1, d) for d in range(nz)]

    def y_copy(which, o):
        ref = xall if which == 0 else call
        return remote(
            ref.at[pl.ds(own_block(o) * tb_size, tb_size)], ref.at[pl.ds((lead + o) * tb_size, tb_size)],
            ys_sem.at[which], yr_sem.at[which, o], at(other, tr, j),
        )

    def cs_copy(z):
        return remote(cs_tx, cs_rx.at[j], css_sem, csr_sem, at(y, tr, z))

    mids = (mid_low, mid_low + 1)

    def token_sums():
        own_load(0, 1).wait()
        for o in range(half):
            x = xall[pl.ds(own_block(o) * tb_size, tb_size), :].astype(F32)
            st_own[o * tb_size:(o + 1) * tb_size, :] = pair_tile(
                jnp.sum(x, axis=1, keepdims=True), jnp.sum(x * x, axis=1, keepdims=True)
            )
        stats = st_own[...].T[0:2]
        st_tx[...] = stats
        st_rx[j] = stats
        for rel, d in stat_list:
            if rel == 0:
                stat_copy(rel, d).start()

    def column_sums(waited):
        ones = jnp.ones((8, depth), BF16)
        for f in range(nfb):
            if f >= waited:
                wu_load(f).wait()
            cs_tx[f:f + 1] = contract(ones, wu[f], 1, 0)[0:1]
        for z in mids:
            @pl.when(j != z)
            def _(z=z):
                cs_copy(z).start()

        @pl.when(is_mid)
        def _():
            cs_rx[j] = cs_tx[...]

        for rel, d in stat_list:
            if rel == 1:
                stat_copy(rel, d).start()
        own_load(1, 1).wait()
        for o in range(half):
            y_copy(1, o).start()
            y_copy(0, o).start()

    def statistics(rel):
        span = st_rx.at[pl.ds(rel * nz, nz - 1 + rel)]
        remote(span, span, ss_sem, sr_sem.at[rel], here).wait_recv()
        total = st_rx[rel * nz]
        for z in range(1, nz):
            total = total + st_rx[rel * nz + z]
        total = total / width
        mean = total[0:1]
        flip[...] = jnp.zeros_like(flip)
        flip[0:1] = mean
        rstd = lax.rsqrt(total[1:2] - mean * mean + EPS)
        flip[1:2] = rstd
        for z in range(nz):
            flip[2 + z:3 + z] = rstd * (st_rx[rel * nz + z][0:1] / depth - mean)
        back = flip[...].T
        if rel == 0:
            ms[0:head] = back[0:head]
            ms[head + rows:] = back[head:]
        else:
            ms[head:head + rows] = back

    def xhat_of(t, span):
        tile = ms[block_rows(t), :]
        x = xall[block_rows(t), span].astype(F32)
        return x, (x - tile[:, 0:1]) * tile[:, 1:2]

    def is_far(t):
        return jnp.logical_and(t >= lead, t < lead + half)

    def norm_rows(t):
        nall[block_rows(t), :] = xhat_of(t, slice(None))[1].astype(BF16)

    def first_statistics():
        statistics(0)

        @pl.when(is_mid)
        def _():
            span = cs_rx.at[pl.ds(0, nz - 1)]
            remote(span, span, css_sem, csr_sem, here).wait_recv()

    def make_rows(t):
        @pl.when(t == 1)
        def _():
            norm_rows(0)

        @pl.when(t == lead)
        def _():
            statistics(1)

        for o in range(half):
            @pl.when(t == lead + o)
            def _(o=o):
                y_copy(1, o).wait_recv()
                y_copy(0, o).wait_recv()

        @pl.when(t > 0)
        def _():
            norm_rows(t)

    def across(s):
        return remote(tx.at[s], rm.at[s], tx_sem, rm_sem.at[lax.rem(s, MID_RING)], at(y, tr, inner))

    def outward(s):
        span = hd.at[:, lax.rem(s, nfb), block_rows(s // nfb)]
        return remote(span, span, hs_sem, hr_sem.at[lax.rem(s, RING)], at(y, tr, outer))

    def partial_stage(s):
        t = s // nfb
        f = lax.rem(s, nfb)

        @pl.when(s < nfb)
        def _():
            wd_load(f).wait()

        @pl.when(f == 0)
        def _():
            make_rows(t)

        parts = parts_of(t, f)

        @pl.when(is_end)
        def _():
            for k in range(2):
                tx[s, k] = parts[k].astype(BF16)
            to_mid(s).start()

        @pl.when(is_mid)
        def _():
            to_mid(s).wait_recv()
            for k in range(2):
                tx[s, k] = (parts[k] + rx[s, k].astype(F32)).astype(BF16)
            across(s).start()

    def act_stage(e):
        across(e).wait_recv()
        f = lax.rem(e, nfb)
        t = e // nfb

        def step(first, i, carry):
            r = pl.ds(pl.multiple_of(i * 16, 16), 16)
            out = pl.ds(pl.multiple_of(t * tb_size + i * 16, 16), 16)
            dhid = tx[e, 0, r, :].astype(F32) + rm[e, 0, r, :].astype(F32)
            pre = tx[e, 1, r, :].astype(F32) + rm[e, 1, r, :].astype(F32)
            if first:
                tile = ms[out, :]
                pre = pre * tile[:, 1:2]
                for z in range(nz):
                    pre = pre + tile[:, 2 + z:3 + z] * cs_rx[z, pl.ds(f, 1), :]
            phi = 0.5 * (1.0 + lax.erf(pre * SQRT_HALF))
            slope = phi + pre * jnp.exp(-0.5 * pre * pre) * INV_SQRT_2PI
            hd[0, f, out, :] = (pre * phi).astype(BF16)
            hd[1, f, out, :] = (dhid * slope).astype(BF16)
            return carry

        for first in (True, False):
            @pl.when((e < nfb) == first)
            def _(first=first):
                lax.fori_loop(0, tb_size // 16, functools.partial(step, first), 0)

        outward(e).start()

    def pair_copy(t):
        return remote(pr_tx.at[t], pr_rx.at[t], prs_sem, prr_sem.at[t], at(y, pair, j))

    def columns(h):
        return pl.ds(pl.multiple_of(h * side, side), side)

    slot = tr * nz + j
    everyone = [(a, b) for a in range(nt) for b in range(nz)]

    def mean_copy(t, o, a, b):
        return remote(
            sq_tx.at[t], sq_rx.at[o, slot], sqs_sem, sqr_sem.at[o], at(y, t_peer(a), z_peer(b))
        )

    def far_mean(t, o):
        return remote(sq_tx.at[t], fm_rx.at[o], fms_sem, fmr_sem.at[o], at(other, tr, j))

    def mean_all(o):
        span = sq_rx.at[o, pl.ds(0, nt * nz - 1)]
        return remote(span, span, sqs_sem, sqr_sem.at[o], here)

    def spread_means(t, o):
        far_mean(t, o).wait_recv()
        sums = sq_tx[t] + fm_rx[o]
        sq_tx[t] = sums
        sq_rx[o, slot] = sums
        for a, b in everyone[1:]:
            mean_copy(t, o, a, b).start()

    def send_means(t):
        xhat = xhat_of(t, slice(None))[1]
        dn = acc[1]
        square[0, 0:tb_size] = pair_tile(
            jnp.sum(dn, axis=1, keepdims=True), jnp.sum(dn * xhat, axis=1, keepdims=True)
        )
        sq_tx[t] = square[0].T[0:2]

        @pl.when(is_far(t))
        def _():
            far_mean(t, t - lead).start()

        @pl.when(t >= lead + half)
        def _():
            spread_means(t, t - half)

    def use_stage(e):
        f = lax.rem(e, nfb)
        t = e // nfb

        @pl.when(is_end)
        def _():
            outward(e).wait_recv()

        @pl.when(f == 0)
        def _():
            acc[...] = jnp.zeros_like(acc)

        acc[0] += contract(hd[0, f, block_rows(t), :], wd[f], 1, 0)
        acc[1] += contract(hd[1, f, block_rows(t), :], wu[f], 1, 1)

        @pl.when(f == nfb - 1)
        def _():
            for k in range(2):
                pr_tx[t, k] = acc[k, :, columns(1 - core)].astype(BF16)
            pair_copy(t).start()
            for k in range(2):
                keep[t, k] = acc[k, :, columns(core)]
            send_means(t)

    def first_rows(f, which):
        cols = pl.ds(pl.multiple_of(f * fb_size, fb_size), fb_size)
        if which == 0:
            grad_down[cols, :] = contract(hd[0, f, 0:rows, :], call[0:rows, :], 0, 0).astype(BF16)
        else:
            grad_up[:, cols] = contract(nall[0:rows, :], hd[1, f, 0:rows, :], 0, 0).astype(BF16)

    def last_rows(f, which):
        cols = pl.ds(pl.multiple_of(f * fb_size, fb_size), fb_size)
        if which == 0:
            part = contract(hd[0, f, rows:, :], call[rows:, :], 0, 0)
            grad_down[cols, :] = (grad_down[cols, :].astype(F32) + part).astype(BF16)
        else:
            part = contract(nall[rows:, :], hd[1, f, rows:, :], 0, 0)
            grad_up[:, cols] = (grad_up[:, cols].astype(F32) + part).astype(BF16)

    def yq_copy(o):
        return remote(y_tx.at[o], y_rx.at[o], yqs_sem, yqr_sem.at[o], at(other, tr, j))

    def cross_copy(o, k):
        return remote(cr_tx.at[o, k], cr_rx.at[o, k], crs_sem, crr_sem.at[o, k], at(y, cross, j))

    def fin_copy(o, k):
        span = fin.at[o, core, k]
        return remote(span, span, fis_sem, fir_sem.at[o], at(y, pair, j))

    def row_sum_stage(t):
        pair_copy(t).wait_recv()
        for k in range(2):
            keep[t, k] += pr_rx[t, k].astype(F32)

        @pl.when(is_far(t))
        def _():
            for k in range(2):
                y_tx[t - lead, k] = keep[t, k].astype(BF16)
            yq_copy(t - lead).start()

    def gather_stage(o):
        t = jnp.where(o < lead, o, o + half)

        @pl.when(o < lead)
        def _():
            spread_means(t, o)

        yq_copy(o).wait_recv()
        for k in range(2):
            cr_tx[o, k] = (keep[t, k] + y_rx[o, k].astype(F32)).astype(BF16)
            cross_copy(o, k).start()

    def total_stage(o):
        for k in range(2):
            cross_copy(o, k).wait_recv()
            fin[o, core, k] = (cr_tx[o, k].astype(F32) + cr_rx[o, k].astype(F32)).astype(BF16)
            fin_copy(o, k).start()

    def finish_stage(o):
        t = jnp.where(o < lead, o, o + half)
        span = fin.at[o, 0]
        remote(span, span, fis_sem, fir_sem.at[o], here).wait_recv()
        mean_all(o).wait_recv()
        total = sq_rx[o, 0]
        for k in range(1, nt * nz):
            total = total + sq_rx[o, k]
        square[1, 0:2] = total / width
        means = square[1].T[0:tb_size]
        rstd = ms[block_rows(t), :][:, 1:2]
        for h in range(2):
            span = slice(h * side, (h + 1) * side)
            x, xhat = xhat_of(t, span)
            mixed[block_rows(o), span] = (x + fin[o, h, 0].astype(F32)).astype(BF16)
            dn = fin[o, h, 1].astype(F32)
            grad[block_rows(o), span] = (
                call[block_rows(t), span].astype(F32)
                + rstd * (dn - means[:, 0:1] - xhat * means[:, 1:2])
            ).astype(BF16)

    pieces = 2 * nfb
    spread = nb // 2 // pieces

    def step(s, carry):
        @pl.when(jnp.logical_and(s == 0, jnp.logical_or(is_mid, is_odd)))
        def _():
            with jax.named_scope("sums"):
                token_sums()

        @pl.when(jnp.logical_and(s == 0, is_mid))
        def _():
            with jax.named_scope("cols"):
                column_sums(0)

        @pl.when(jnp.logical_and(jnp.logical_and(s > 0, s <= COLS_AT), is_end))
        def _():
            wu_load(s).wait()

        @pl.when(jnp.logical_and(s == nfb, is_end))
        def _():
            with jax.named_scope("norm"):
                first_statistics()

        @pl.when(jnp.logical_and(s < nb, jnp.logical_or(is_mid, s > 0)))
        def _():
            with jax.named_scope("partial"):
                partial_stage(s)

        @pl.when(jnp.logical_and(s == SUMS_AT, jnp.logical_and(is_end, jnp.logical_not(is_odd))))
        def _():
            with jax.named_scope("sums"):
                token_sums()

        @pl.when(jnp.logical_and(s == COLS_AT, is_end))
        def _():
            with jax.named_scope("cols"):
                column_sums(COLS_AT + 1)

        e = s - lag
        valid = jnp.logical_and(e >= 0, e < nb)

        @pl.when(jnp.logical_and(e == 0, is_mid))
        def _():
            with jax.named_scope("norm"):
                first_statistics()

        @pl.when(jnp.logical_and(valid, is_mid))
        def _():
            with jax.named_scope("act"):
                act_stage(e)

        @pl.when(valid)
        def _():
            with jax.named_scope("use"):
                use_stage(e)

        g = e - nb // 2

        @pl.when(jnp.logical_and(g >= 0, jnp.logical_and(g < nb // 2, lax.rem(g, spread) == 0)))
        def _():
            with jax.named_scope("first"):
                p = g // spread

                @pl.when(p < nfb)
                def _():
                    first_rows(p, 0)

                @pl.when(p >= nfb)
                def _():
                    first_rows(p - nfb, 1)

        def done_block(shift, stage):
            k = e - shift - (nfb - 1)
            t = k // nfb

            @pl.when(jnp.logical_and(jnp.logical_and(k >= 0, t < ntb - 1), lax.rem(k, nfb) == 0))
            def _():
                stage(t)

        def gather_at(t):
            first = jnp.logical_and(t > lead, t <= half)

            @pl.when(jnp.logical_or(first, t >= half + lead))
            def _():
                with jax.named_scope("gather"):
                    gather_stage(jnp.where(first, t - lead - 1, t - half))

        def total_at(t):
            @pl.when(jnp.logical_and(t > lead, t <= half))
            def _():
                total_stage(t - lead - 1)

        done_block(ROW_SHIFT, row_sum_stage)
        done_block(ROW_SHIFT + 1, gather_at)
        done_block(ROW_SHIFT + 6, total_at)
        return carry

    lax.fori_loop(0, nb + max(END_LAG, MID_LAG), step, 0)

    def last_piece(which, low, high):
        def body(f, carry):
            last_rows(f, which)
            return carry

        lax.fori_loop(low, high, body, 0)

    def finish_step(o, carry):
        finish_stage(o)
        return carry

    def total_step(o, carry):
        total_stage(o)
        return carry

    with jax.named_scope("rowsum"):
        row_sum_stage(ntb - 1)
    with jax.named_scope("gather"):
        gather_stage(half - 1)
    with jax.named_scope("total"):
        lax.fori_loop(lead, half - 1, total_step, 0)
    with jax.named_scope("finish"):
        lax.fori_loop(0, lead, finish_step, 0)
    with jax.named_scope("last"):
        last_piece(0, 0, nfb)
        last_piece(1, 0, nfb // 2)
    with jax.named_scope("total"):
        total_stage(half - 1)
    with jax.named_scope("last"):
        last_piece(1, nfb // 2, nfb)
    with jax.named_scope("finish"):
        lax.fori_loop(lead, half, finish_step, 0)

    def sent(ref, sem):
        remote(ref, ref, sem, sem, here).wait_send()

    with jax.named_scope("drain"):
        sent(st_rx.at[pl.ds(1, 2 * nz - 1)], ss_sem)
    far = pl.ds(head, rows)
    sent(xall.at[far], ys_sem.at[0])
    sent(call.at[far], ys_sem.at[1])
    sent(tx, tx_sem)

    @pl.when(is_end)
    def _():
        sent(cs_rx.at[pl.ds(0, 2)], css_sem)

    @pl.when(is_mid)
    def _():
        sent(cs_rx.at[0], css_sem)


    @pl.when(is_mid)
    def _():
        sent(hd, hs_sem)

    sent(pr_tx, prs_sem)
    sent(y_tx, yqs_sem)
    sent(cr_tx, crs_sem)
    sent(fin.at[:, 0], fis_sem)
    sent(sq_rx.at[:, pl.ds(0, nt * nz - 1)], sqs_sem)
    sent(fm_rx, fms_sem)


def line_call(nz, nt, tokens, w_up, w_down, cotangent):
    rows, depth = tokens.shape
    ff = w_up.shape[1]
    tb, fb = 64, FB_SIZE
    nfb = ff // fb
    ntb = 2 * rows // tb
    half = ntb // 2
    nb = nfb * ntb
    side = depth // 2
    sums = -(-nfb // 8) * 8
    vm = pltpu.VMEM
    dma = pltpu.SemaphoreType.DMA
    big = (nb, 2, tb, fb)
    scratch = [
        vm((2 * rows, depth), BF16), vm((2 * rows, depth), BF16), vm((2 * rows, depth), BF16),
        vm((sums, fb), F32), vm((nz, sums, fb), F32),
        vm((nfb, depth, fb), BF16), vm((nfb, fb, depth), BF16),
        vm(big, BF16), vm(big, BF16), vm(big, BF16), vm((2, nfb, 2 * rows, fb), BF16),
        vm((rows, 128), F32), vm((2, rows), F32), vm((2 * nz, 2, rows), F32), vm((128, rows), F32),
        vm((2 * rows, 128), F32),
        vm((2, tb, depth), F32),
        vm((ntb, 2, tb, side), BF16), vm((ntb, 2, tb, side), BF16), vm((ntb, 2, tb, side), F32),
        vm((half, 2, tb, side), BF16), vm((half, 2, tb, side), BF16),
        vm((half, 2, tb, side), BF16), vm((half, 2, tb, side), BF16), vm((half, 2, 2, tb, side), BF16),
        vm((2, 128, 128), F32), vm((ntb, 2, 128), F32), vm((half, nt * nz, 2, 128), F32), vm((half, 2, 128), F32),
        dma((2, 2)), dma((nfb,)), dma((nfb,)),
        dma, dma((RING,)), dma((MID_RING,)), dma, dma((RING,)),
        dma, dma((2,)), dma((2,)), dma((2, half)),
        dma, dma((ntb,)), dma, dma((half,)),
        dma, dma((half, 2)), dma, dma((half,)), dma, dma((half,)), dma, dma, dma, dma((half,)),
    ]
    return pl.pallas_call(
        functools.partial(line_kernel, (nz, nt, rows, depth, ff, tb, fb)),
        out_shape=tuple(
            OUT(shape, BF16)
            for shape in ((rows, depth), (rows, depth), (depth, ff), (ff, depth))
        ),
        in_specs=[pl.BlockSpec(memory_space=pl.ANY)] * 4,
        out_specs=[pl.BlockSpec(memory_space=pltpu.VMEM)] * 4,
        scratch_shapes=scratch,
        compiler_params=pltpu.CompilerParams(
            collective_id=0, has_side_effects=True, vmem_limit_bytes=VMEM_LIMIT
        ),
    )(tokens, w_up, w_down, cotangent)


def write_kernel(*refs):
    n = len(refs) // 2
    sems = refs[-1]
    copies = []
    for k in range(n):
        rows = refs[k].shape[0]
        cuts = CUTS if rows * refs[k].shape[1] > 1 << 20 else 1
        for c in range(cuts):
            span = pl.ds(c * (rows // cuts), rows // cuts)
            copies.append((refs[k].at[span], refs[n + k].at[span]))
    copies = [pltpu.make_async_copy(a, b, sems.at[i]) for i, (a, b) in enumerate(copies)]
    for copy in copies:
        copy.start()
    for copy in copies:
        copy.wait()


def write_out(arrays):
    return pl.pallas_call(
        write_kernel,
        out_shape=tuple(jax.ShapeDtypeStruct(a.shape, a.dtype) for a in arrays),
        in_specs=[pl.BlockSpec(memory_space=pltpu.VMEM)] * len(arrays),
        out_specs=[pl.BlockSpec(memory_space=pl.ANY)] * len(arrays),
        scratch_shapes=[pltpu.SemaphoreType.DMA((4 * CUTS,))],
        compiler_params=pltpu.CompilerParams(vmem_limit_bytes=WRITE_LIMIT),
    )(*arrays)


def local_line(tokens, w_up, w_down, cotangent):
    nz = lax.axis_size("tcol")
    nt = lax.axis_size("trow")
    return write_out(line_call(nz, nt, tokens, w_up, w_down, cotangent))


def local_plain(tokens, w_up, w_down, cotangent):
    width = tokens.shape[1] * lax.axis_size("tcol")
    input_float = tokens.astype(F32)
    cot_all = lax.all_gather(cotangent, "fsdp", axis=0, tiled=True)
    sum_one, sum_two = lax.psum(
        (jnp.sum(input_float, axis=1), jnp.sum(input_float * input_float, axis=1)), "tcol"
    )
    token_mean = sum_one / width
    var = sum_two / width - token_mean * token_mean
    inverse_stddev = lax.rsqrt(var + EPS)
    centered_scaled = (input_float - token_mean[:, None]) * inverse_stddev[:, None]
    normalized_rows = centered_scaled.astype(BF16)
    normed_all = lax.all_gather(normalized_rows, "fsdp", axis=0, tiled=True)
    dhid_part = contract(cot_all, w_down, 1, 1).astype(BF16)
    dhid = lax.psum_scatter(dhid_part, "tcol", scatter_dimension=0, tiled=True).astype(F32)
    pre_part = contract(normed_all, w_up, 1, 0).astype(BF16)
    pre = lax.psum_scatter(pre_part, "tcol", scatter_dimension=0, tiled=True).astype(F32)
    hidden = lax.all_gather(gelu_value(pre).astype(BF16), "tcol", axis=0, tiled=True)
    dpre = lax.all_gather((dhid * gelu_slope(pre)).astype(BF16), "tcol", axis=0, tiled=True)
    branch_part = contract(hidden, w_down, 1, 0).astype(BF16)
    branch = lax.psum_scatter(branch_part, "fsdp", scatter_dimension=0, tiled=True)
    branch = lax.psum(branch, "trow").astype(F32)
    mixed = (input_float + branch).astype(BF16)
    grad_down = contract(hidden, cot_all, 0, 0).astype(BF16)
    dnorm_part = contract(dpre, w_up, 1, 1).astype(BF16)
    dnorm = lax.psum_scatter(dnorm_part, "fsdp", scatter_dimension=0, tiled=True)
    normed_gradient = lax.psum(dnorm, "trow").astype(F32)
    grad_up = contract(normed_all, dpre, 0, 0).astype(BF16)
    mean_first, mean_second = lax.psum(
        (jnp.sum(normed_gradient, axis=1), jnp.sum(normed_gradient * centered_scaled, axis=1)),
        "tcol",
    )
    first_moment = mean_first / width
    second_moment = mean_second / width
    input_gradient = cotangent.astype(F32) + inverse_stddev[:, None] * (
        normed_gradient - first_moment[:, None] - centered_scaled * second_moment[:, None]
    )
    return (mixed, input_gradient.astype(BF16), grad_up, grad_down)


def solution(mesh):
    fits = mesh.shape["fsdp"] == 2 and mesh.shape["trow"] == 4 and mesh.shape["tcol"] == 4
    return jax.shard_map(
        local_line if fits else local_plain,
        mesh=mesh,
        in_specs=(
            P("fsdp", "tcol"),
            P("tcol", ("fsdp", "trow")),
            P(("fsdp", "trow"), "tcol"),
            P("fsdp", "tcol"),
        ),
        out_specs=(
            P("fsdp", "tcol"),
            P("fsdp", "tcol"),
            P("tcol", ("fsdp", "trow")),
            P(("fsdp", "trow"), "tcol"),
        ),
        check_vma=False,
    )
```

```python
import functools

import jax
import jax.numpy as jnp
from jax import lax
from jax.experimental import pallas as pl
from jax.experimental.pallas import tpu as pltpu
from jax.sharding import PartitionSpec as P

MESH = pl.DeviceIdType.MESH
BF16 = jnp.bfloat16
F32 = jnp.float32
SQRT_HALF = 0.7071067811865476
INV_SQRT_2PI = 0.3989422804014327
EPS = 1e-05
END_LAG = 12
MID_LAG = 3
ROW_SHIFT = 4
RING = 15
MID_RING = 10
COLS_AT = 3
CUTS = 4
SUMS_AT = 1
FB_SIZE = 256
VMEM_LIMIT = 46 * 1024 * 1024
WRITE_LIMIT = 1024 * 1024
OUT = pltpu.VMEM


def gelu_value(pre):
    phi = 0.5 * (1.0 + jax.scipy.special.erf(pre * SQRT_HALF))
    return pre * phi


def gelu_slope(pre):
    phi = 0.5 * (1.0 + jax.scipy.special.erf(pre * SQRT_HALF))
    return phi + pre * jnp.exp(-0.5 * pre * pre) * INV_SQRT_2PI


def contract(left, right, left_dim, right_dim):
    return lax.dot_general(
        left, right, (((left_dim,), (right_dim,)), ((), ())), preferred_element_type=F32
    )


def line_kernel(
    sizes,
    tok_in, up_in, down_in, cot_in,
    mixed, grad, grad_up, grad_down,
    xall, call, nall, cs_tx, cs_rx, wu, wd, tx, rx, rm, hd,
    st_own, st_tx, st_rx, flip, ms, acc, pr_tx, pr_rx, keep, y_tx, y_rx, cr_tx, cr_rx, fin, square, sq_tx, sq_rx, fm_rx,
    load_sem, wu_sem, wd_sem, tx_sem, rx_sem, rm_sem, hs_sem, hr_sem,
    ss_sem, sr_sem, ys_sem, yr_sem, prs_sem, prr_sem, yqs_sem, yqr_sem, crs_sem, crr_sem, fis_sem, fir_sem,
    sqs_sem, sqr_sem, css_sem, csr_sem, fms_sem, fmr_sem,
):
    nz, nt, rows, depth, ff, tb_size, fb_size = sizes
    nfb = ff // fb_size
    ntb = 2 * rows // tb_size
    half = ntb // 2
    lead = half // 2
    nb = ntb * nfb
    side = depth // 2
    width = depth * nz
    y = lax.axis_index("fsdp")
    tr = lax.axis_index("trow")
    j = lax.axis_index("tcol")
    mid_low = nz // 2 - 1
    is_mid = jnp.logical_or(j == mid_low, j == mid_low + 1)
    is_end = jnp.logical_not(is_mid)
    core = lax.rem(tr, 2)
    is_odd = core == 1
    pair = tr + 1 - 2 * core
    cross = lax.rem(tr + nt // 2, nt)
    inner = jnp.where(j <= mid_low, j + 1, j - 1)
    outer = jnp.where(j <= mid_low, jnp.maximum(j - 1, 0), jnp.minimum(j + 1, nz - 1))
    lag = jnp.where(is_mid, MID_LAG, END_LAG)
    other = 1 - y

    def at(yy, tt, jj):
        return {"fsdp": yy, "trow": tt, "tcol": jj}

    def remote(src, dst, send, recv, device):
        return pltpu.make_async_remote_copy(
            src_ref=src, dst_ref=dst, send_sem=send, recv_sem=recv,
            device_id=device, device_id_type=MESH,
        )

    def z_peer(d):
        return lax.rem(j + d, nz)

    def t_peer(d):
        return lax.rem(tr + d, nt)

    here = at(y, tr, j)

    def own_block(o):
        return o if o < lead else o + half

    def block_rows(t):
        return pl.ds(pl.multiple_of(t * tb_size, tb_size), tb_size)

    head = lead * tb_size
    spans = [(pl.ds(0, head), pl.ds(0, head)), (pl.ds(head, rows - head), pl.ds(head + rows, rows - head))]

    def own_load(which, part):
        source, dest = (tok_in, xall) if which == 0 else (cot_in, call)
        return pltpu.make_async_copy(
            source.at[spans[part][0]], dest.at[spans[part][1]], load_sem.at[which, part]
        )

    def wd_load(f):
        return pltpu.make_async_copy(
            down_in.at[pl.ds(pl.multiple_of(f * fb_size, fb_size), fb_size)], wd.at[f], wd_sem.at[f]
        )

    def wu_load(f):
        return pltpu.make_async_copy(
            up_in.at[:, pl.ds(pl.multiple_of(f * fb_size, fb_size), fb_size)], wu.at[f], wu_sem.at[f]
        )

    own_load(1, 0).start()
    own_load(0, 0).start()
    wd_load(0).start()
    wu_load(0).start()

    barrier = pltpu.get_barrier_semaphore()
    partners = [(y, t_peer(a), z_peer(b)) for a in range(nt) for b in range(nz) if a or b]
    partners += [(other, tr, z_peer(b)) for b in range(nz)]
    for device in partners:
        pl.semaphore_signal(barrier, inc=1, device_id=at(*device), device_id_type=MESH)

    lane = lax.broadcasted_iota(jnp.int32, (tb_size, 128), 1)

    def pair_tile(one, two):
        return jnp.where(lane == 0, one, jnp.where(lane == 1, two, 0.0))

    own_load(0, 1).start()
    for f in range(1, nfb):
        wu_load(f).start()
        wd_load(f).start()
    own_load(1, 1).start()
    square[...] = jnp.zeros_like(square)
    sq_tx[...] = jnp.zeros_like(sq_tx)
    own_load(1, 0).wait()
    own_load(0, 0).wait()

    x = xall[0:tb_size, :].astype(F32)
    nall[0:tb_size, :] = (x - jnp.sum(x, axis=1, keepdims=True) / depth).astype(BF16)

    def parts_of(t, f):
        return (
            contract(call[block_rows(t), :], wd[f], 1, 1),
            contract(nall[block_rows(t), :], wu[f], 1, 0),
        )

    def to_mid(s):
        return remote(tx.at[s], rx.at[s], tx_sem, rx_sem.at[lax.rem(s, RING)], at(y, tr, inner))

    @pl.when(is_end)
    def _():
        wd_load(0).wait()
        wu_load(0).wait()
        parts = parts_of(0, 0)
        for k in range(2):
            tx[0, k] = parts[k].astype(BF16)

    pl.semaphore_wait(barrier, len(partners))

    @pl.when(is_end)
    def _():
        to_mid(0).start()

    def stat_copy(rel, d):
        target = at(y if rel == 0 else other, tr, z_peer(d))
        return remote(st_tx, st_rx.at[rel * nz + j], ss_sem, sr_sem.at[rel], target)

    stat_list = [(0, d) for d in range(1, nz)] + [(1, d) for d in range(nz)]

    def y_copy(which, o):
        ref = xall if which == 0 else call
        return remote(
            ref.at[pl.ds(own_block(o) * tb_size, tb_size)], ref.at[pl.ds((lead + o) * tb_size, tb_size)],
            ys_sem.at[which], yr_sem.at[which, o], at(other, tr, j),
        )

    def cs_copy(z):
        return remote(cs_tx, cs_rx.at[j], css_sem, csr_sem, at(y, tr, z))

    mids = (mid_low, mid_low + 1)

    def token_sums():
        own_load(0, 1).wait()
        for o in range(half):
            x = xall[pl.ds(own_block(o) * tb_size, tb_size), :].astype(F32)
            st_own[o * tb_size:(o + 1) * tb_size, :] = pair_tile(
                jnp.sum(x, axis=1, keepdims=True), jnp.sum(x * x, axis=1, keepdims=True)
            )
        stats = st_own[...].T[0:2]
        st_tx[...] = stats
        st_rx[j] = stats
        for rel, d in stat_list:
            if rel == 0:
                stat_copy(rel, d).start()

    def column_sums(waited):
        ones = jnp.ones((8, depth), BF16)
        for f in range(nfb):
            if f >= waited:
                wu_load(f).wait()
            cs_tx[f:f + 1] = contract(ones, wu[f], 1, 0)[0:1]
        for z in mids:
            @pl.when(j != z)
            def _(z=z):
                cs_copy(z).start()

        @pl.when(is_mid)
        def _():
            cs_rx[j] = cs_tx[...]

        for rel, d in stat_list:
            if rel == 1:
                stat_copy(rel, d).start()
        own_load(1, 1).wait()
        for o in range(half):
            y_copy(1, o).start()
            y_copy(0, o).start()

    def statistics(rel):
        span = st_rx.at[pl.ds(rel * nz, nz - 1 + rel)]
        remote(span, span, ss_sem, sr_sem.at[rel], here).wait_recv()
        total = st_rx[rel * nz]
        for z in range(1, nz):
            total = total + st_rx[rel * nz + z]
        total = total / width
        mean = total[0:1]
        flip[...] = jnp.zeros_like(flip)
        flip[0:1] = mean
        rstd = lax.rsqrt(total[1:2] - mean * mean + EPS)
        flip[1:2] = rstd
        for z in range(nz):
            flip[2 + z:3 + z] = rstd * (st_rx[rel * nz + z][0:1] / depth - mean)
        back = flip[...].T
        if rel == 0:
            ms[0:head] = back[0:head]
            ms[head + rows:] = back[head:]
        else:
            ms[head:head + rows] = back

    def xhat_of(t, span):
        tile = ms[block_rows(t), :]
        x = xall[block_rows(t), span].astype(F32)
        return x, (x - tile[:, 0:1]) * tile[:, 1:2]

    def is_far(t):
        return jnp.logical_and(t >= lead, t < lead + half)

    def norm_rows(t):
        nall[block_rows(t), :] = xhat_of(t, slice(None))[1].astype(BF16)

    def first_statistics():
        statistics(0)

        @pl.when(is_mid)
        def _():
            span = cs_rx.at[pl.ds(0, nz - 1)]
            remote(span, span, css_sem, csr_sem, here).wait_recv()

    def make_rows(t):
        @pl.when(t == 1)
        def _():
            norm_rows(0)

        @pl.when(t == lead)
        def _():
            statistics(1)

        for o in range(half):
            @pl.when(t == lead + o)
            def _(o=o):
                y_copy(1, o).wait_recv()
                y_copy(0, o).wait_recv()

        @pl.when(t > 0)
        def _():
            norm_rows(t)

    def across(s):
        return remote(tx.at[s], rm.at[s], tx_sem, rm_sem.at[lax.rem(s, MID_RING)], at(y, tr, inner))

    def outward(s):
        span = hd.at[:, lax.rem(s, nfb), block_rows(s // nfb)]
        return remote(span, span, hs_sem, hr_sem.at[lax.rem(s, RING)], at(y, tr, outer))

    def partial_stage(s):
        t = s // nfb
        f = lax.rem(s, nfb)

        @pl.when(s < nfb)
        def _():
            wd_load(f).wait()

        @pl.when(f == 0)
        def _():
            make_rows(t)

        parts = parts_of(t, f)

        @pl.when(is_end)
        def _():
            for k in range(2):
                tx[s, k] = parts[k].astype(BF16)
            to_mid(s).start()

        @pl.when(is_mid)
        def _():
            to_mid(s).wait_recv()
            for k in range(2):
                tx[s, k] = (parts[k] + rx[s, k].astype(F32)).astype(BF16)
            across(s).start()

    def act_stage(e):
        across(e).wait_recv()
        f = lax.rem(e, nfb)
        t = e // nfb

        def step(first, i, carry):
            r = pl.ds(pl.multiple_of(i * 16, 16), 16)
            out = pl.ds(pl.multiple_of(t * tb_size + i * 16, 16), 16)
            dhid = tx[e, 0, r, :].astype(F32) + rm[e, 0, r, :].astype(F32)
            pre = tx[e, 1, r, :].astype(F32) + rm[e, 1, r, :].astype(F32)
            if first:
                tile = ms[out, :]
                pre = pre * tile[:, 1:2]
                for z in range(nz):
                    pre = pre + tile[:, 2 + z:3 + z] * cs_rx[z, pl.ds(f, 1), :]
            phi = 0.5 * (1.0 + lax.erf(pre * SQRT_HALF))
            slope = phi + pre * jnp.exp(-0.5 * pre * pre) * INV_SQRT_2PI
            hd[0, f, out, :] = (pre * phi).astype(BF16)
            hd[1, f, out, :] = (dhid * slope).astype(BF16)
            return carry

        for first in (True, False):
            @pl.when((e < nfb) == first)
            def _(first=first):
                lax.fori_loop(0, tb_size // 16, functools.partial(step, first), 0)

        outward(e).start()

    def pair_copy(t):
        return remote(pr_tx.at[t], pr_rx.at[t], prs_sem, prr_sem.at[t], at(y, pair, j))

    def columns(h):
        return pl.ds(pl.multiple_of(h * side, side), side)

    slot = tr * nz + j
    everyone = [(a, b) for a in range(nt) for b in range(nz)]

    def mean_copy(t, o, a, b):
        return remote(
            sq_tx.at[t], sq_rx.at[o, slot], sqs_sem, sqr_sem.at[o], at(y, t_peer(a), z_peer(b))
        )

    def far_mean(t, o):
        return remote(sq_tx.at[t], fm_rx.at[o], fms_sem, fmr_sem.at[o], at(other, tr, j))

    def mean_all(o):
        span = sq_rx.at[o, pl.ds(0, nt * nz - 1)]
        return remote(span, span, sqs_sem, sqr_sem.at[o], here)

    def spread_means(t, o):
        far_mean(t, o).wait_recv()
        sums = sq_tx[t] + fm_rx[o]
        sq_tx[t] = sums
        sq_rx[o, slot] = sums
        for a, b in everyone[1:]:
            mean_copy(t, o, a, b).start()

    def send_means(t):
        xhat = xhat_of(t, slice(None))[1]
        dn = acc[1]
        square[0, 0:tb_size] = pair_tile(
            jnp.sum(dn, axis=1, keepdims=True), jnp.sum(dn * xhat, axis=1, keepdims=True)
        )
        sq_tx[t] = square[0].T[0:2]

        @pl.when(is_far(t))
        def _():
            far_mean(t, t - lead).start()

        @pl.when(t >= lead + half)
        def _():
            spread_means(t, t - half)

    def use_stage(e):
        f = lax.rem(e, nfb)
        t = e // nfb

        @pl.when(is_end)
        def _():
            outward(e).wait_recv()

        @pl.when(f == 0)
        def _():
            acc[...] = jnp.zeros_like(acc)

        acc[0] += contract(hd[0, f, block_rows(t), :], wd[f], 1, 0)
        acc[1] += contract(hd[1, f, block_rows(t), :], wu[f], 1, 1)

        @pl.when(f == nfb - 1)
        def _():
            for k in range(2):
                pr_tx[t, k] = acc[k, :, columns(1 - core)].astype(BF16)
            pair_copy(t).start()
            for k in range(2):
                keep[t, k] = acc[k, :, columns(core)]
            send_means(t)

    def first_rows(f, which):
        cols = pl.ds(pl.multiple_of(f * fb_size, fb_size), fb_size)
        if which == 0:
            grad_down[cols, :] = contract(hd[0, f, 0:rows, :], call[0:rows, :], 0, 0).astype(BF16)
        else:
            grad_up[:, cols] = contract(nall[0:rows, :], hd[1, f, 0:rows, :], 0, 0).astype(BF16)

    def last_rows(f, which):
        cols = pl.ds(pl.multiple_of(f * fb_size, fb_size), fb_size)
        if which == 0:
            part = contract(hd[0, f, rows:, :], call[rows:, :], 0, 0)
            grad_down[cols, :] = (grad_down[cols, :].astype(F32) + part).astype(BF16)
        else:
            part = contract(nall[rows:, :], hd[1, f, rows:, :], 0, 0)
            grad_up[:, cols] = (grad_up[:, cols].astype(F32) + part).astype(BF16)

    def yq_copy(o):
        return remote(y_tx.at[o], y_rx.at[o], yqs_sem, yqr_sem.at[o], at(other, tr, j))

    def cross_copy(o, k):
        return remote(cr_tx.at[o, k], cr_rx.at[o, k], crs_sem, crr_sem.at[o, k], at(y, cross, j))

    def fin_copy(o, k):
        span = fin.at[o, core, k]
        return remote(span, span, fis_sem, fir_sem.at[o], at(y, pair, j))

    def row_sum_stage(t):
        pair_copy(t).wait_recv()
        for k in range(2):
            keep[t, k] += pr_rx[t, k].astype(F32)

        @pl.when(is_far(t))
        def _():
            for k in range(2):
                y_tx[t - lead, k] = keep[t, k].astype(BF16)
            yq_copy(t - lead).start()

    def gather_stage(o):
        t = jnp.where(o < lead, o, o + half)

        @pl.when(o < lead)
        def _():
            spread_means(t, o)

        yq_copy(o).wait_recv()
        for k in range(2):
            cr_tx[o, k] = (keep[t, k] + y_rx[o, k].astype(F32)).astype(BF16)
            cross_copy(o, k).start()

    def total_stage(o):
        for k in range(2):
            cross_copy(o, k).wait_recv()
            fin[o, core, k] = (cr_tx[o, k].astype(F32) + cr_rx[o, k].astype(F32)).astype(BF16)
            fin_copy(o, k).start()

    def finish_stage(o):
        t = jnp.where(o < lead, o, o + half)
        span = fin.at[o, 0]
        remote(span, span, fis_sem, fir_sem.at[o], here).wait_recv()
        mean_all(o).wait_recv()
        total = sq_rx[o, 0]
        for k in range(1, nt * nz):
            total = total + sq_rx[o, k]
        square[1, 0:2] = total / width
        means = square[1].T[0:tb_size]
        rstd = ms[block_rows(t), :][:, 1:2]
        for h in range(2):
            span = slice(h * side, (h + 1) * side)
            x, xhat = xhat_of(t, span)
            mixed[block_rows(o), span] = (x + fin[o, h, 0].astype(F32)).astype(BF16)
            dn = fin[o, h, 1].astype(F32)
            grad[block_rows(o), span] = (
                call[block_rows(t), span].astype(F32)
                + rstd * (dn - means[:, 0:1] - xhat * means[:, 1:2])
            ).astype(BF16)

    pieces = 2 * nfb
    spread = nb // 2 // pieces

    def step(s, carry):
        @pl.when(jnp.logical_and(s == 0, jnp.logical_or(is_mid, is_odd)))
        def _():
            with jax.named_scope("sums"):
                token_sums()

        @pl.when(jnp.logical_and(s == 0, is_mid))
        def _():
            with jax.named_scope("cols"):
                column_sums(0)

        @pl.when(jnp.logical_and(jnp.logical_and(s > 0, s <= COLS_AT), is_end))
        def _():
            wu_load(s).wait()

        @pl.when(jnp.logical_and(s == nfb, is_end))
        def _():
            with jax.named_scope("norm"):
                first_statistics()

        @pl.when(jnp.logical_and(s < nb, jnp.logical_or(is_mid, s > 0)))
        def _():
            with jax.named_scope("partial"):
                partial_stage(s)

        @pl.when(jnp.logical_and(s == SUMS_AT, jnp.logical_and(is_end, jnp.logical_not(is_odd))))
        def _():
            with jax.named_scope("sums"):
                token_sums()

        @pl.when(jnp.logical_and(s == COLS_AT, is_end))
        def _():
            with jax.named_scope("cols"):
                column_sums(COLS_AT + 1)

        e = s - lag
        valid = jnp.logical_and(e >= 0, e < nb)

        @pl.when(jnp.logical_and(e == 0, is_mid))
        def _():
            with jax.named_scope("norm"):
                first_statistics()

        @pl.when(jnp.logical_and(valid, is_mid))
        def _():
            with jax.named_scope("act"):
                act_stage(e)

        @pl.when(valid)
        def _():
            with jax.named_scope("use"):
                use_stage(e)

        g = e - nb // 2

        @pl.when(jnp.logical_and(g >= 0, jnp.logical_and(g < nb // 2, lax.rem(g, spread) == 0)))
        def _():
            with jax.named_scope("first"):
                p = g // spread

                @pl.when(p < nfb)
                def _():
                    first_rows(p, 0)

                @pl.when(p >= nfb)
                def _():
                    first_rows(p - nfb, 1)

        def done_block(shift, stage):
            k = e - shift - (nfb - 1)
            t = k // nfb

            @pl.when(jnp.logical_and(jnp.logical_and(k >= 0, t < ntb - 1), lax.rem(k, nfb) == 0))
            def _():
                stage(t)

        def gather_at(t):
            first = jnp.logical_and(t > lead, t <= half)

            @pl.when(jnp.logical_or(first, t >= half + lead))
            def _():
                with jax.named_scope("gather"):
                    gather_stage(jnp.where(first, t - lead - 1, t - half))

        def total_at(t):
            @pl.when(jnp.logical_and(t > lead, t <= half))
            def _():
                total_stage(t - lead - 1)

        done_block(ROW_SHIFT, row_sum_stage)
        done_block(ROW_SHIFT + 1, gather_at)
        done_block(ROW_SHIFT + 6, total_at)
        return carry

    lax.fori_loop(0, nb + max(END_LAG, MID_LAG), step, 0)

    def last_piece(which, low, high):
        def body(f, carry):
            last_rows(f, which)
            return carry

        lax.fori_loop(low, high, body, 0)

    def finish_step(o, carry):
        finish_stage(o)
        return carry

    def total_step(o, carry):
        total_stage(o)
        return carry

    with jax.named_scope("rowsum"):
        row_sum_stage(ntb - 1)
    with jax.named_scope("gather"):
        gather_stage(half - 1)
    with jax.named_scope("finish"):
        lax.fori_loop(0, lead, finish_step, 0)
    with jax.named_scope("last"):
        last_piece(0, 0, nfb)
        last_piece(1, 0, nfb // 2)
    with jax.named_scope("total"):
        lax.fori_loop(lead, half, total_step, 0)
    with jax.named_scope("last"):
        last_piece(1, nfb // 2, nfb)
    with jax.named_scope("finish"):
        lax.fori_loop(lead, half, finish_step, 0)

    def sent(ref, sem):
        remote(ref, ref, sem, sem, here).wait_send()

    with jax.named_scope("drain"):
        sent(st_rx.at[pl.ds(1, 2 * nz - 1)], ss_sem)
    far = pl.ds(head, rows)
    sent(xall.at[far], ys_sem.at[0])
    sent(call.at[far], ys_sem.at[1])
    sent(tx, tx_sem)

    @pl.when(is_end)
    def _():
        sent(cs_rx.at[pl.ds(0, 2)], css_sem)

    @pl.when(is_mid)
    def _():
        sent(cs_rx.at[0], css_sem)


    @pl.when(is_mid)
    def _():
        sent(hd, hs_sem)

    sent(pr_tx, prs_sem)
    sent(y_tx, yqs_sem)
    sent(cr_tx, crs_sem)
    sent(fin.at[:, 0], fis_sem)
    sent(sq_rx.at[:, pl.ds(0, nt * nz - 1)], sqs_sem)
    sent(fm_rx, fms_sem)


def line_call(nz, nt, tokens, w_up, w_down, cotangent):
    rows, depth = tokens.shape
    ff = w_up.shape[1]
    tb, fb = 64, FB_SIZE
    nfb = ff // fb
    ntb = 2 * rows // tb
    half = ntb // 2
    nb = nfb * ntb
    side = depth // 2
    sums = -(-nfb // 8) * 8
    vm = pltpu.VMEM
    dma = pltpu.SemaphoreType.DMA
    big = (nb, 2, tb, fb)
    scratch = [
        vm((2 * rows, depth), BF16), vm((2 * rows, depth), BF16), vm((2 * rows, depth), BF16),
        vm((sums, fb), F32), vm((nz, sums, fb), F32),
        vm((nfb, depth, fb), BF16), vm((nfb, fb, depth), BF16),
        vm(big, BF16), vm(big, BF16), vm(big, BF16), vm((2, nfb, 2 * rows, fb), BF16),
        vm((rows, 128), F32), vm((2, rows), F32), vm((2 * nz, 2, rows), F32), vm((128, rows), F32),
        vm((2 * rows, 128), F32),
        vm((2, tb, depth), F32),
        vm((ntb, 2, tb, side), BF16), vm((ntb, 2, tb, side), BF16), vm((ntb, 2, tb, side), F32),
        vm((half, 2, tb, side), BF16), vm((half, 2, tb, side), BF16),
        vm((half, 2, tb, side), BF16), vm((half, 2, tb, side), BF16), vm((half, 2, 2, tb, side), BF16),
        vm((2, 128, 128), F32), vm((ntb, 2, 128), F32), vm((half, nt * nz, 2, 128), F32), vm((half, 2, 128), F32),
        dma((2, 2)), dma((nfb,)), dma((nfb,)),
        dma, dma((RING,)), dma((MID_RING,)), dma, dma((RING,)),
        dma, dma((2,)), dma((2,)), dma((2, half)),
        dma, dma((ntb,)), dma, dma((half,)),
        dma, dma((half, 2)), dma, dma((half,)), dma, dma((half,)), dma, dma, dma, dma((half,)),
    ]
    return pl.pallas_call(
        functools.partial(line_kernel, (nz, nt, rows, depth, ff, tb, fb)),
        out_shape=tuple(
            OUT(shape, BF16)
            for shape in ((rows, depth), (rows, depth), (depth, ff), (ff, depth))
        ),
        in_specs=[pl.BlockSpec(memory_space=pl.ANY)] * 4,
        out_specs=[pl.BlockSpec(memory_space=pltpu.VMEM)] * 4,
        scratch_shapes=scratch,
        compiler_params=pltpu.CompilerParams(
            collective_id=0, has_side_effects=True, vmem_limit_bytes=VMEM_LIMIT
        ),
    )(tokens, w_up, w_down, cotangent)


def write_kernel(*refs):
    n = len(refs) // 2
    sems = refs[-1]
    copies = []
    for k in range(n):
        rows = refs[k].shape[0]
        cuts = CUTS if rows * refs[k].shape[1] > 1 << 20 else 1
        for c in range(cuts):
            span = pl.ds(c * (rows // cuts), rows // cuts)
            copies.append((refs[k].at[span], refs[n + k].at[span]))
    copies = [pltpu.make_async_copy(a, b, sems.at[i]) for i, (a, b) in enumerate(copies)]
    for copy in copies:
        copy.start()
    for copy in copies:
        copy.wait()


def write_out(arrays):
    return pl.pallas_call(
        write_kernel,
        out_shape=tuple(jax.ShapeDtypeStruct(a.shape, a.dtype) for a in arrays),
        in_specs=[pl.BlockSpec(memory_space=pltpu.VMEM)] * len(arrays),
        out_specs=[pl.BlockSpec(memory_space=pl.ANY)] * len(arrays),
        scratch_shapes=[pltpu.SemaphoreType.DMA((4 * CUTS,))],
        compiler_params=pltpu.CompilerParams(vmem_limit_bytes=WRITE_LIMIT),
    )(*arrays)


def local_line(tokens, w_up, w_down, cotangent):
    nz = lax.axis_size("tcol")
    nt = lax.axis_size("trow")
    return write_out(line_call(nz, nt, tokens, w_up, w_down, cotangent))


def local_plain(tokens, w_up, w_down, cotangent):
    width = tokens.shape[1] * lax.axis_size("tcol")
    input_float = tokens.astype(F32)
    cot_all = lax.all_gather(cotangent, "fsdp", axis=0, tiled=True)
    sum_one, sum_two = lax.psum(
        (jnp.sum(input_float, axis=1), jnp.sum(input_float * input_float, axis=1)), "tcol"
    )
    token_mean = sum_one / width
    var = sum_two / width - token_mean * token_mean
    inverse_stddev = lax.rsqrt(var + EPS)
    centered_scaled = (input_float - token_mean[:, None]) * inverse_stddev[:, None]
    normalized_rows = centered_scaled.astype(BF16)
    normed_all = lax.all_gather(normalized_rows, "fsdp", axis=0, tiled=True)
    dhid_part = contract(cot_all, w_down, 1, 1).astype(BF16)
    dhid = lax.psum_scatter(dhid_part, "tcol", scatter_dimension=0, tiled=True).astype(F32)
    pre_part = contract(normed_all, w_up, 1, 0).astype(BF16)
    pre = lax.psum_scatter(pre_part, "tcol", scatter_dimension=0, tiled=True).astype(F32)
    hidden = lax.all_gather(gelu_value(pre).astype(BF16), "tcol", axis=0, tiled=True)
    dpre = lax.all_gather((dhid * gelu_slope(pre)).astype(BF16), "tcol", axis=0, tiled=True)
    branch_part = contract(hidden, w_down, 1, 0).astype(BF16)
    branch = lax.psum_scatter(branch_part, "fsdp", scatter_dimension=0, tiled=True)
    branch = lax.psum(branch, "trow").astype(F32)
    mixed = (input_float + branch).astype(BF16)
    grad_down = contract(hidden, cot_all, 0, 0).astype(BF16)
    dnorm_part = contract(dpre, w_up, 1, 1).astype(BF16)
    dnorm = lax.psum_scatter(dnorm_part, "fsdp", scatter_dimension=0, tiled=True)
    normed_gradient = lax.psum(dnorm, "trow").astype(F32)
    grad_up = contract(normed_all, dpre, 0, 0).astype(BF16)
    mean_first, mean_second = lax.psum(
        (jnp.sum(normed_gradient, axis=1), jnp.sum(normed_gradient * centered_scaled, axis=1)),
        "tcol",
    )
    first_moment = mean_first / width
    second_moment = mean_second / width
    input_gradient = cotangent.astype(F32) + inverse_stddev[:, None] * (
        normed_gradient - first_moment[:, None] - centered_scaled * second_moment[:, None]
    )
    return (mixed, input_gradient.astype(BF16), grad_up, grad_down)


def solution(mesh):
    fits = mesh.shape["fsdp"] == 2 and mesh.shape["trow"] == 4 and mesh.shape["tcol"] == 4
    return jax.shard_map(
        local_line if fits else local_plain,
        mesh=mesh,
        in_specs=(
            P("fsdp", "tcol"),
            P("tcol", ("fsdp", "trow")),
            P(("fsdp", "trow"), "tcol"),
            P("fsdp", "tcol"),
        ),
        out_specs=(
            P("fsdp", "tcol"),
            P("fsdp", "tcol"),
            P("tcol", ("fsdp", "trow")),
            P(("fsdp", "trow"), "tcol"),
        ),
        check_vma=False,
    )
```
